256 devices in a mesh: dp: 64 (over z, y, core), mp: 4 (over x).
Axes of the slice: x: 4, y: 4, z: 8, core: 2. Of those that a mesh axis runs over, the one named last changes fastest.
Arguments:
- hidden: bfloat16 [128, 64, 3584], P('dp', None, 'mp'), may hold values from -6 to 6
- rewards: float32 [128, 64], P('dp'), may hold values from -6 to 6
- actions: int32 [128, 64], P('dp'), may hold values from 0 to 152063, as said below
- lengths: int32 [128], P('dp'), may hold values from 1 to 64, 4096 in all
- table: bfloat16 [152064, 3584], P('dp', 'mp'), may hold values from -0.09375 to 0.09375
- q_one: bfloat16 [3584, 3584], P('dp', 'mp'), may hold values from -0.09375 to 0.09375
- q_two: bfloat16 [3584, 3584], P('dp', 'mp'), may hold values from -0.09375 to 0.09375
- t_one: bfloat16 [3584, 3584], P('dp', 'mp'), may hold values from -0.09375 to 0.09375
- t_two: bfloat16 [3584, 3584], P('dp', 'mp'), may hold values from -0.09375 to 0.09375
- value_weight: bfloat16 [3584], P('mp'), may hold values from -0.09375 to 0.09375
- value_bias: float32 [1], replicated, may hold values from -3 to 3
Outputs:
- loss: float32 [], replicated
- grad_q_one: float32 [3584, 3584], P('dp', 'mp')
- grad_q_two: float32 [3584, 3584], P('dp', 'mp')
- grad_value: float32 [3584], P('mp')
- grad_bias: float32 [1], replicated
- target_one: bfloat16 [3584, 3584], P('dp', 'mp')
- target_two: bfloat16 [3584, 3584], P('dp', 'mp')
The draws below stay inside these ranges and needn't reach their ends.
Inputs may be any that keep to these rules, and one draw needn't show every extreme that they name: `actions`: among the 128 positions of the prompts of one index of dp, exactly 2 action ids fall in each of the aligned blocks of 2376 vocabulary rows.
All inputs are finite; a program needn't handle non-finite values. No bound on the sum of `lengths` on one device may be relied on, other than what follows from the above.
Results may differ from the reference program's by a relative error of at most 0.0045.
Values may be sent and summed in bfloat16 or wider, within the bound.
No kernel may reach another device: no remote copies, remote signals or barrier semaphores. Data moves between devices by JAX's collectives and lax.ppermute only.
A program may use at most 192 MiB of HBM per device.

```python
import math
import jax
import jax.numpy as jnp
import numpy as np
from jax import lax

D = 3584
V = 152064
DH = 3584
PR_DEV = 2
SLOT = 64
PROMPTS = 128


def draw_actions(key, part):
    blocks = PROMPTS // PR_DEV
    per_block = PR_DEV * SLOT
    row_count = V // blocks
    keys_split = jax.random.split(jax.random.fold_in(key, 11), blocks)

    def shuffle(block_key):
        return jax.random.permutation(block_key, per_block)
    shuffled = jax.vmap(shuffle)(keys_split)
    holders = shuffled % blocks
    offsets = jax.random.randint(jax.random.fold_in(key, 12), (blocks, per_block), 0, row_count)
    return (holders * row_count + offsets).astype(jnp.int32).reshape(PROMPTS, SLOT)


def steps_of(key, shape, pieces, least, largest):
    factor_of = 1.0
    for dim, blocks in pieces:
        steps = jax.random.uniform(jax.random.fold_in(jax.random.fold_in(key, 6), dim), (blocks,), jnp.float32, least / len(pieces), largest / len(pieces))
        factor_of = factor_of * jnp.repeat(jnp.exp(steps), shape[dim] // blocks).reshape((-1,) + (1,) * (len(shape) - 1 - dim))
    return factor_of


def profile(count, total, most, lean):
    weights = [(1 << 20) // math.isqrt(grade ** lean) + 1 for grade in range(2, count + 1)]
    surplus, holding = total - most - (count - 1), [1] * (count - 1)
    while surplus > 0:
        candidates = [i for i in range(count - 1) if holding[i] < most]
        mass, left = sum([weights[i] for i in candidates]), surplus
        for i in candidates:
            more = min(most - holding[i], max(1, left * weights[i] // mass), surplus)
            holding[i] = holding[i] + more
            surplus = surplus - more
    return np.array([most] + holding)


def uneven_parts(own_key, count, total, limit, lean):
    if count == 2:
        one = jax.random.randint(own_key, (), max(1, total - limit), min(limit, total - 1) + 1)
        return jnp.stack([one, total - one])
    tallies = jnp.asarray(profile(count, total, limit, lean), jnp.int32)
    twos = (count - 1) // 2
    source_of, sink = tallies[1:1 + 2 * twos:2], tallies[2:2 + 2 * twos:2]
    slack = jnp.minimum(source_of - 1, limit - sink)
    moved = jax.random.randint(jax.random.fold_in(own_key, 1), (twos,), 0, 1 << 20) % (slack + 1)
    tallies = tallies.at[1:1 + 2 * twos:2].set(source_of - moved).at[2:2 + 2 * twos:2].set(sink + moved)
    return tallies[jax.random.permutation(jax.random.fold_in(own_key, 2), count)]


def scatter_about(key, shape, deviation, most, shards=(), kind=jnp.bfloat16):
    entries = deviation * jax.random.normal(key, shape, jnp.float32)
    if shards:
        entries = entries * steps_of(key, shape, shards, -0.22, 0.18)
    return jnp.clip(entries, -most, most).astype(kind)


def setup_inputs(seed: int = 0) -> dict:
    seeds = jax.random.split(jax.random.key(seed), 12)
    hidden = scatter_about(seeds[0], (PROMPTS, SLOT, D), 1.0, 6.0, ((0, 64), (2, 4)))
    rewards = scatter_about(seeds[1], (PROMPTS, SLOT), 1.0, 6.0, ((0, 64),), jnp.float32)
    actions = draw_actions(jax.random.fold_in(seeds[11], 71), 0)
    lengths = uneven_parts(seeds[3], PROMPTS, PROMPTS * SLOT // 2, SLOT, 2).astype(jnp.int32)
    table = scatter_about(seeds[4], (V, DH), DH ** -0.5, 0.09375, ((0, 64), (1, 4)))
    q_one = scatter_about(seeds[5], (D, DH), D ** -0.5, 0.09375, ((0, 64), (1, 4)))
    q_two = scatter_about(seeds[6], (D, DH), D ** -0.5, 0.09375, ((0, 64), (1, 4)))
    t_one = scatter_about(seeds[7], (D, DH), D ** -0.5, 0.09375, ((0, 64), (1, 4)))
    t_two = scatter_about(seeds[8], (D, DH), D ** -0.5, 0.09375, ((0, 64), (1, 4)))
    value_weight = scatter_about(seeds[9], (D,), D ** -0.5, 0.09375, ((0, 4),))
    value_bias = scatter_about(seeds[10], (1,), 1.0, 3.0, (), jnp.float32)
    return dict(hidden=hidden, rewards=rewards, actions=actions, lengths=lengths, table=table, q_one=q_one, q_two=q_two, t_one=t_one, t_two=t_two, value_weight=value_weight, value_bias=value_bias)


discount = 0.99
expectile = 0.7
polyak_rate = 0.005

def head_gelu(inputs):
    return jax.nn.gelu(inputs, approximate=True)

def slope(preact, upstream):
    _, pullback = jax.vjp(head_gelu, preact)
    return pullback(upstream)[0]

def critic_terms(q_first, q_second, t_first, t_second, values, rewards, lengths):
    positions = jnp.arange(values.shape[1], dtype=jnp.int32)[None, :]
    valid = positions < lengths[:, None]
    follows = positions + 1 < lengths[:, None]
    shifted = jnp.concatenate([values[:, 1:], jnp.zeros_like(values[:, :1])], axis=1)
    target = rewards + discount * jnp.where(follows, shifted, 0.0)
    lowest = jnp.minimum(t_first, t_second)
    spread = lowest - values
    weights = jnp.where(spread < 0.0, 1.0 - expectile, expectile)
    err_one = q_first - target
    err_two = q_second - target
    loss_sum = jnp.sum(jnp.where(valid, err_one * err_one + err_two * err_two + weights * spread * spread, 0.0))
    grad_first = jnp.where(valid, 2.0 * err_one, 0.0)
    grad_second = jnp.where(valid, 2.0 * err_two, 0.0)
    grad_values = jnp.where(valid, -2.0 * weights * spread, 0.0)
    return (grad_first, grad_second, grad_values, loss_sum)

def reference(hidden, rewards, actions, lengths, table, q_one, q_two, t_one, t_two, value_weight, value_bias):
    blocks = PROMPTS // PR_DEV
    total_count = jnp.sum(lengths).astype(jnp.float32)

    def one_block(carry, inputs):
        acc_one, acc_two, acc_value, acc_bias, acc_loss = carry
        block_hidden, block_rewards, block_actions, block_lengths = inputs
        flat = block_hidden.reshape(PR_DEV * SLOT, D)
        embed = table[block_actions.reshape(-1)].astype(jnp.float32)
        preacts = [jnp.dot(flat, weight, preferred_element_type=jnp.float32) for weight in (q_one, q_two, t_one, t_two)]
        scores = [lax.optimization_barrier(jnp.sum(head_gelu(preact) * embed, axis=1)).reshape(PR_DEV, SLOT) for preact in preacts]
        values = jnp.dot(flat, value_weight, preferred_element_type=jnp.float32).reshape(PR_DEV, SLOT) + value_bias[0]
        grad_first, grad_second, grad_values, loss_sum = critic_terms(scores[0], scores[1], scores[2], scores[3], values, block_rewards, block_lengths)
        back_one = slope(preacts[0], grad_first.reshape(-1, 1) * embed).astype(jnp.bfloat16)
        back_two = slope(preacts[1], grad_second.reshape(-1, 1) * embed).astype(jnp.bfloat16)
        dims = (((0,), (0,)), ((), ()))
        acc_one = acc_one + lax.dot_general(flat, back_one, dims, preferred_element_type=jnp.float32)
        acc_two = acc_two + lax.dot_general(flat, back_two, dims, preferred_element_type=jnp.float32)
        acc_value = acc_value + jnp.dot(grad_values.reshape(-1), flat.astype(jnp.float32), precision=lax.Precision.HIGHEST)
        acc_bias = acc_bias + jnp.sum(grad_values)
        acc_loss = acc_loss + loss_sum
        return ((acc_one, acc_two, acc_value, acc_bias, acc_loss), None)
    start = (jnp.zeros((D, DH), jnp.float32), jnp.zeros((D, DH), jnp.float32), jnp.zeros((D,), jnp.float32), jnp.zeros((), jnp.float32), jnp.zeros((), jnp.float32))
    inputs = (hidden.reshape(blocks, PR_DEV, SLOT, D), rewards.reshape(blocks, PR_DEV, SLOT), actions.reshape(blocks, PR_DEV, SLOT), lengths.reshape(blocks, PR_DEV))
    final, _ = lax.scan(one_block, start, inputs)
    acc_one, acc_two, acc_value, acc_bias, acc_loss = final
    new_one = ((1.0 - polyak_rate) * t_one.astype(jnp.float32) + polyak_rate * q_one.astype(jnp.float32)).astype(jnp.bfloat16)
    new_two = ((1.0 - polyak_rate) * t_two.astype(jnp.float32) + polyak_rate * q_two.astype(jnp.float32)).astype(jnp.bfloat16)
    return (acc_loss / total_count, acc_one / total_count, acc_two / total_count, acc_value / total_count, (acc_bias / total_count).reshape(1), new_one, new_two)
```

```python
import jax
import jax.numpy as jnp
from jax import lax
from jax.sharding import Mesh
from jax.sharding import PartitionSpec as P

discount = 0.99
expectile = 0.7
polyak_rate = 0.005

ZS, YS, CS, XS = 8, 4, 2, 4
ROWS = ("z", "y", "c")
f32 = jnp.float32
bf16 = jnp.bfloat16


def exchange(pieces, axes):
    return lax.all_to_all(pieces, axes, split_axis=0, concat_axis=0, tiled=True)


def to_all(shard, axes):
    return exchange(jnp.broadcast_to(shard, (lax.axis_size(axes), *shard.shape)), axes)


def swapped(a):
    return lax.ppermute(a, "c", ((0, 1), (1, 0)))


def head_gelu(inputs):
    return jax.nn.gelu(inputs, approximate=True)


def slope(preact, upstream):
    _, pullback = jax.vjp(head_gelu, preact)
    return pullback(upstream)[0]


def critic_terms(q_first, q_second, t_first, t_second, values, rewards, lengths):
    positions = jnp.arange(values.shape[1], dtype=f32)[None, :]
    valid = positions < lengths[:, None]
    follows = positions + 1 < lengths[:, None]
    shifted = jnp.concatenate([values[:, 1:], jnp.zeros_like(values[:, :1])], axis=1)
    target = rewards + discount * jnp.where(follows, shifted, 0.0)
    lowest = jnp.minimum(t_first, t_second)
    spread = lowest - values
    weights = jnp.where(spread < 0.0, 1.0 - expectile, expectile)
    err_one = q_first - target
    err_two = q_second - target
    loss_sum = jnp.sum(
        jnp.where(valid, err_one * err_one + err_two * err_two + weights * spread * spread, 0.0)
    )
    grad_first = jnp.where(valid, 2.0 * err_one, 0.0)
    grad_second = jnp.where(valid, 2.0 * err_two, 0.0)
    grad_values = jnp.where(valid, -2.0 * weights * spread, 0.0)
    return (grad_first, grad_second, grad_values, loss_sum)


def split_thrice(a):
    first = a.astype(bf16)
    rest = a - first.astype(f32)
    second = rest.astype(bf16)
    third = (rest - second.astype(f32)).astype(bf16)
    return (first, second, third)


def lookup(ids, table):
    count = ids.shape[0]
    local_rows = table.shape[0]
    holders = lax.axis_size(ROWS)
    per_holder = count // holders
    columns = table.shape[1] // YS
    place = jnp.arange(count, dtype=jnp.int32)
    holder = ids // local_rows
    local = ids % local_rows
    earlier = (holder[:, None] == holder[None, :]) & (place[None, :] < place[:, None])
    slot = per_holder * holder + jnp.sum(earlier.astype(jnp.int32), axis=1)
    coded = local + 4096 * place
    asked = jnp.sum(jnp.where(slot[:, None] == place[None, :], coded[:, None], 0), axis=0)
    got = exchange(asked.reshape(holders, per_holder), ROWS).reshape(count)
    found = table[got & 4095]
    where = (got >> 12).astype(bf16)
    found = found.reshape(ZS, YS, CS, per_holder, YS, columns).transpose(0, 4, 2, 1, 3, 5)
    where = jnp.broadcast_to(
        where.reshape(ZS, 1, YS, CS, per_holder, 1).transpose(0, 1, 3, 2, 4, 5),
        (ZS, YS, CS, YS, per_holder, 1),
    )
    sent = jnp.concatenate([found, where], axis=-1).reshape(holders, YS * per_holder, columns + 1)
    back = exchange(sent, ROWS).reshape(holders * YS * per_holder, columns + 1)
    slots = jnp.arange(holders * YS * per_holder, dtype=jnp.int32)
    token = (slots // per_holder % YS) * count + back[:, columns].astype(jnp.int32)
    one_hot = (token[:, None] == jnp.arange(YS * count, dtype=jnp.int32)[None, :]).astype(bf16)
    return lax.dot_general(
        one_hot, back[:, :columns], (((0,), (0,)), ((), ())), preferred_element_type=f32
    ).astype(bf16)


def on_device(
    hidden, rewards, actions, lengths, table, q_one, q_two, t_one, t_two, value_weight, value_bias
):
    prompts, slots, width = hidden.shape
    tokens = prompts * slots
    core = lax.axis_index("c")
    share, head_cols = q_one.shape
    cols = head_cols // YS
    local = hidden.reshape(tokens, width)

    heads = jnp.stack([jnp.stack([q_one, t_one]), jnp.stack([q_two, t_two])])
    pieces = heads.reshape(CS, 2, share, YS, cols).transpose(3, 0, 2, 1, 4)
    pieces = exchange(pieces.reshape(YS * CS, share, 2 * cols), ("y", "c"))
    weights = lax.all_gather(
        pieces.reshape(YS * CS * share, 2 * cols), "z", axis=0, tiled=True
    ).reshape(XS, width, 2 * cols)

    own = to_all(local, ("y", "x")).reshape(YS, XS, tokens, width)
    other = swapped(own)
    embed_own = lookup(actions.reshape(tokens), table)
    embed_other = swapped(embed_own)

    def forward(states):
        return jnp.einsum("yxtk,xkn->ytn", states, weights, preferred_element_type=f32).reshape(
            YS * tokens, 2 * cols
        )

    pre_own, pre_other = forward(own), forward(other)

    def scores(pre, embed):
        e = embed.astype(f32)
        return (
            jnp.sum(head_gelu(pre[:, :cols]) * e, axis=1).reshape(YS, tokens),
            jnp.sum(head_gelu(pre[:, cols:]) * e, axis=1).reshape(YS, tokens),
        )

    q_own, t_own = scores(pre_own, embed_own)
    q_other, t_other = scores(pre_other, embed_other)
    value_part = jnp.dot(local, value_weight, preferred_element_type=f32)

    def by_core(a, b):
        return jnp.where(core == 0, jnp.stack([a, b]), jnp.stack([b, a]))

    message = jnp.concatenate(
        [
            by_core(q_own, q_other).reshape(-1),
            by_core(t_own, t_other).reshape(-1),
            value_part,
            rewards.reshape(-1),
            jnp.repeat(lengths.astype(f32), slots),
        ]
    ).reshape(-1, tokens)
    said = to_all(message, ("y", "c", "x")).reshape(YS, CS, XS, -1, tokens)
    summed = jnp.sum(said[..., : 4 * CS * YS, :], axis=(0, 2))
    group = CS * YS
    q_first, q_second = summed[0, :group], summed[1, :group]
    t_first, t_second = summed[0, group : 2 * group], summed[1, group : 2 * group]

    def by_place(a):
        return a.transpose(1, 0, 2).reshape(group, tokens)

    values = by_place(jnp.sum(said[..., 2 * group, :], axis=2)) + value_bias[0]
    all_rewards = by_place(said[:, :, 0, 2 * group + 1, :])
    all_lengths = by_place(said[:, :, 0, 2 * group + 2, :])

    def prompts_of(a):
        return a.reshape(group * prompts, slots)

    grad_first, grad_second, grad_values, loss_sum = critic_terms(
        prompts_of(q_first),
        prompts_of(q_second),
        prompts_of(t_first),
        prompts_of(t_second),
        prompts_of(values),
        prompts_of(all_rewards),
        prompts_of(all_lengths)[:, 0],
    )
    my_grad = jnp.where(core == 0, grad_first, grad_second).reshape(CS, -1)
    grad_values = grad_values.reshape(CS, -1)

    def own_and_other(a):
        return jnp.where(core == 0, a[0], a[1]), jnp.where(core == 0, a[1], a[0])

    g_own, g_other = own_and_other(my_grad)
    e_own, e_other = own_and_other(grad_values)

    def back(pre, embed, g, e):
        d = slope(pre[:, :cols], g[:, None] * embed.astype(f32)).astype(bf16)
        return jnp.concatenate([d, jnp.stack(split_thrice(e), axis=1)], axis=1).reshape(
            YS, tokens, cols + 3
        )

    def against(states, d):
        return jnp.einsum("yxtk,ytn->xkn", states, d, preferred_element_type=f32)

    grads = against(own, back(pre_own, embed_own, g_own, e_own)) + against(
        other, back(pre_other, embed_other, g_other, e_other)
    )
    group_count = jnp.sum(prompts_of(all_lengths)[:, 0])
    terms = grads[..., :cols].astype(bf16).reshape(ZS * YS * CS, share, cols)
    value_terms = jnp.sum(
        lax.dynamic_index_in_dim(grads[..., cols:], lax.axis_index("x"), 0, keepdims=False), axis=1
    )
    totals = jnp.concatenate(
        [value_terms, jnp.stack([jnp.sum(grad_values), loss_sum, group_count])]
    )
    totals = jnp.sum(to_all(totals, "z"), axis=0)
    factor = 1.0 / totals[width + 2]
    value_grad = totals[:width] * factor
    bias_grad = totals[width] * factor
    loss_total = totals[width + 1] * factor

    landed = exchange(terms, ROWS).reshape(ZS, YS, CS, share, cols)
    head_grads = jnp.sum(landed.astype(f32), axis=0) * factor
    head_grads = head_grads.transpose(1, 2, 0, 3).reshape(CS, share, head_cols)

    new_one = (
        (1.0 - polyak_rate) * t_one.astype(f32) + polyak_rate * q_one.astype(f32)
    ).astype(bf16)
    new_two = (
        (1.0 - polyak_rate) * t_two.astype(f32) + polyak_rate * q_two.astype(f32)
    ).astype(bf16)
    return (
        loss_total,
        head_grads[0],
        head_grads[1],
        value_grad,
        bias_grad.reshape(1),
        new_one,
        new_two,
    )


def solution(mesh):
    fine = Mesh(mesh.devices.reshape(ZS, YS, CS, XS), ("z", "y", "c", "x"))
    in_specs = (
        P(ROWS, None, "x"),
        P(ROWS, None),
        P(ROWS, None),
        P(ROWS),
        P(ROWS, "x"),
        P(ROWS, "x"),
        P(ROWS, "x"),
        P(ROWS, "x"),
        P(ROWS, "x"),
        P("x"),
        P(),
    )
    out_specs = (P(), P(ROWS, "x"), P(ROWS, "x"), P("x"), P(), P(ROWS, "x"), P(ROWS, "x"))
    return jax.shard_map(
        on_device, mesh=fine, in_specs=in_specs, out_specs=out_specs, check_vma=False
    )
```

```python
import functools

import jax
import jax.numpy as jnp
from jax import lax
from jax.experimental import pallas as pl
from jax.experimental.pallas import tpu as pltpu
from jax.sharding import Mesh
from jax.sharding import PartitionSpec as P


discount = 0.99
expectile = 0.7
polyak_rate = 0.005

ZS, YS, CS, XS = 8, 4, 2, 4
ROWS = ("z", "y", "c")
f32 = jnp.float32
bf16 = jnp.bfloat16
VMEM = pltpu.VMEM
root = 0.7978845608028654
cubic = 0.044715


def exchange(pieces, axes):
    return lax.all_to_all(pieces, axes, split_axis=0, concat_axis=0, tiled=True)


def ahead(a, axis, steps):
    n = lax.axis_size(axis)
    return lax.ppermute(a, axis, tuple(((i + steps) % n, i) for i in range(n)))


def sum_over(a, axis):
    n = lax.axis_size(axis)
    return sum([ahead(a, axis, s) for s in range(1, n)], a)


def split_thrice(a):
    first = a.astype(bf16)
    rest = a - first.astype(f32)
    second = rest.astype(bf16)
    third = (rest - second.astype(f32)).astype(bf16)
    return (first, second, third)


def repack_kernel(place, one, two, three, four, hidden, *outs):
    sent, half_a, half_b, out = outs[:YS], *outs[YS:]
    cols = out.shape[2] // 4
    share = one.shape[0]
    for h, ref in enumerate((one, two, three, four)):
        for y in range(YS):
            out[y, :, h * cols : (h + 1) * cols] = ref[:, y * cols : (y + 1) * cols]
    for r in range(YS):
        sent[r][...] = out[lax.rem(place[0] + YS - r, YS)]
    for half, ref in enumerate((half_a, half_b)):
        for z2 in range(ZS // XS):
            for y in range(YS):
                for c in range(CS):
                    old = ((z2 * YS + y) * CS + c) * share
                    new = ((z2 * CS + c) * YS + y) * share
                    ref[:, new : new + share] = hidden[half, :, old : old + share]


def gather_kernel(place, *refs):
    for r in range(YS):
        refs[YS][lax.rem(place[0] + r, YS)] = refs[r][...]


def forward_kernel(place, *refs):
    a_refs, b_refs = refs[:YS], refs[YS : YS + XS]
    weights, embed_in, extras = refs[YS + XS : YS + XS + 3]
    pre_out, states_out, said = refs[YS + XS + 3 : YS + XS + 6]
    pre, states, embed, held, sems, part_sems, more = refs[YS + XS + 6 :]
    y, x = place[0], place[1]
    slot_count = a_refs[0].shape[1]
    tokens = 2 * slot_count
    heads_width = weights.shape[2]

    def load(xr):
        return pltpu.make_async_copy(weights.at[lax.rem(x + xr, XS)], held.at[xr], sems.at[xr])

    def parts(xr):
        found = []
        for r in range(YS):
            low = pl.ds(r * tokens, slot_count)
            high = pl.ds(r * tokens + slot_count, slot_count)
            for half, (source, to) in enumerate(((a_refs[r].at[xr], low), (b_refs[xr].at[r], high))):
                found.append(
                    pltpu.make_async_copy(source, states.at[xr, to], part_sems.at[xr, r, half])
                )
        return found

    for xr in range(XS):
        load(xr).start()
        for copy in parts(xr):
            copy.start()
    fetch = pltpu.make_async_copy(embed_in, embed, more.at[0])
    fetch.start()
    keep_states = pltpu.make_async_copy(states, states_out, more.at[1])
    for xr in range(XS):
        for copy in parts(xr):
            copy.wait()
        if xr == XS - 1:
            keep_states.start()
        load(xr).wait()

        def columns(at):
            part = jnp.dot(states[xr], held[xr, :, at], preferred_element_type=f32)
            pre[:, at] = part if xr == 0 else pre[:, at] + part

        whole = heads_width // 256

        @pl.loop(0, whole)
        def _(n):
            columns(pl.ds(pl.multiple_of(n * 256, 256), 256))

        if heads_width > whole * 256:
            columns(slice(whole * 256, heads_width))

    cols = heads_width // 4
    keep_pre = pltpu.make_async_copy(pre.at[:, : pre_out.shape[1]], pre_out, more.at[2])
    keep_pre.start()
    fetch.wait()

    @pl.loop(0, YS)
    def _(r):
        rows = pl.ds(pl.multiple_of(r * tokens, tokens), tokens)
        total = extras[...]
        for n in range(heads_width // 128):
            lanes = slice(n * 128, (n + 1) * 128)
            p = pre[rows, lanes]
            g = 0.5 * p * (1.0 + jnp.tanh(root * (p + cubic * (p * p * p))))
            g = g * embed[rows, lanes].astype(f32)
            lane = lax.broadcasted_iota(jnp.int32, (8, 128), 1) + n * 128
            head = lax.broadcasted_iota(jnp.int32, (8, 128), 0)
            chosen = ((lane >= head * cols) & (lane < (head + 1) * cols)).astype(f32).astype(bf16)
            for piece in split_thrice(g):
                total = total + lax.dot_general(
                    chosen, piece, (((1,), (1,)), ((), ())), preferred_element_type=f32
                )
        for copy in range(YS * XS):
            said[copy, lax.rem(y + r, YS)] = total

    keep_states.wait()
    keep_pre.wait()


def backward_kernel(
    place, bias, said, pre_in, embed_in, states_in, keep, send, small, value, *scratch
):
    pre, embed, states, held, grads, sems, more = scratch

    def load(xr):
        return pltpu.make_async_copy(states_in.at[xr], states.at[xr], sems.at[xr])

    fetch_pre = pltpu.make_async_copy(pre_in, pre, more.at[0])
    fetch_embed = pltpu.make_async_copy(embed_in.at[:, : embed.shape[1]], embed, more.at[1])
    fetch_pre.start()
    fetch_embed.start()
    for xr in range(XS):
        load(xr).start()
    y, x, core = place[0], place[1], place[2]
    tokens = said.shape[4]
    width = states.shape[2]
    share = width // (ZS // XS * YS * CS)
    cols = width // YS
    both = 2 * cols
    slot = lax.rem(lax.broadcasted_iota(jnp.int32, (1, tokens), 1), tokens // 2).astype(f32)
    row = lax.broadcasted_iota(jnp.int32, (8, tokens), 0)
    value[...] = jnp.zeros_like(value)
    fetch_pre.wait()
    fetch_embed.wait()
    load(0).wait()

    def prompts(r, sums):
        bias_sum, loss_sum, count_sum = sums
        ya = lax.rem(y + r, YS)
        scores = said[0, 0, ya]
        for i in range(1, YS * XS):
            scores = scores + said[i // XS, i % XS, ya]
        mine = said[ya, 0, 0]
        values = mine[4:5]
        for i in range(1, XS):
            values = values + said[ya, i, 0][4:5]
        values = values + bias[0]
        rewards, length = mine[5:6], mine[6:7]
        valid = slot < length
        following = pltpu.roll(values, tokens - 1, 1)
        target = rewards + discount * jnp.where(slot + 1.0 < length, following, 0.0)
        spread = jnp.minimum(scores[2:3], scores[3:4]) - values
        weights = jnp.where(spread < 0.0, 1.0 - expectile, expectile)
        err_one = scores[0:1] - target
        err_two = scores[1:2] - target
        loss_sum = loss_sum + jnp.where(
            valid, err_one * err_one + err_two * err_two + weights * spread * spread, 0.0
        )
        g_one = jnp.where(valid, 2.0 * err_one, 0.0)
        g_two = jnp.where(valid, 2.0 * err_two, 0.0)
        e = jnp.where(valid, -2.0 * weights * spread, 0.0)
        bias_sum = bias_sum + e
        count_sum = count_sum + jnp.where(slot == 0.0, length, 0.0)
        first = e.astype(bf16).astype(f32)
        second = (e - first).astype(bf16).astype(f32)
        third = e - first - second
        thirds = jnp.where(row == 0, first, jnp.where(row == 1, second, third))
        thirds = jnp.where(row < 3, thirds, 0.0).astype(bf16)
        rows = pl.ds(pl.multiple_of(r * tokens, tokens), tokens)
        value[...] = value[...] + jnp.dot(thirds, states[0, rows], preferred_element_type=f32)
        upright = jnp.transpose(jnp.where(row == 0, g_one, jnp.where(row == 1, g_two, 0.0)))
        left, right = upright[:, 0:1], upright[:, 1:2]
        for n in range(held.shape[1] // 128):
            lanes = slice(n * 128, (n + 1) * 128)
            lane = lax.broadcasted_iota(jnp.int32, (tokens, 128), 1) + n * 128
            g = jnp.where(lane < cols, left, jnp.where(lane < both, right, 0.0))
            p = pre[rows, lanes]
            t = jnp.tanh(root * (p + cubic * (p * p * p)))
            steep = 0.5 * (1.0 + t) + 0.5 * p * (1.0 - t * t) * (
                root * (1.0 + 3.0 * cubic * (p * p))
            )
            held[rows, lanes] = (g * embed[rows, lanes].astype(f32) * steep).astype(bf16)
        return bias_sum, loss_sum, count_sum

    nothing = jnp.zeros((1, tokens), f32)
    bias_sum, loss_sum, count_sum = lax.fori_loop(0, YS, prompts, (nothing, nothing, nothing))
    small[...] = jnp.where(
        row == 0, bias_sum, jnp.where(row == 1, loss_sum, jnp.where(row == 2, count_sum, 0.0))
    )

    @pl.loop(0, XS)
    def _(xr):
        xa = lax.rem(x + xr, XS)

        @pl.when(xr > 0)
        def _():
            load(xr).wait()

        for n in range(held.shape[1] // 256):
            lanes = slice(n * 256, (n + 1) * 256)
            grads[:, lanes] = lax.dot_general(
                states[xr],
                held[:, lanes],
                (((0,), (0,)), ((), ())),
                preferred_element_type=f32,
            )
        for z2 in range(ZS // XS):
            for yy in range(YS):
                to = xa * (ZS // XS) + z2
                low = (z2 * CS * YS + yy) * share
                high = low + YS * share
                for n in range(both // 128):
                    lanes = slice(n * 128, (n + 1) * 128)
                    rows = slice(n * share, (n + 1) * share)
                    first, second = grads[low : low + share, lanes], grads[high : high + share, lanes]
                    keep[to, yy, rows] = jnp.where(core == 0, first, second)
                    send[to, yy, rows] = jnp.where(core == 0, second, first).astype(bf16)
                lanes = slice(both // 128 * 128, both)
                rows = slice(both // 128 * share, None)
                first, second = grads[low : low + share, lanes], grads[high : high + share, lanes]
                mine = jnp.where(core == 0, first, second)
                theirs = jnp.where(core == 0, second, first)
                keep[to, yy, rows] = jnp.concatenate([mine[:32], mine[share - 32 :]], axis=1)
                send[to, yy, rows] = jnp.concatenate(
                    [theirs[:32], theirs[share - 32 :]], axis=1
                ).astype(bf16)


def finish_kernel(*refs):
    totals, landed, one, two, value, rest = refs[:ZS], *refs[ZS:]
    summed = totals[0][...]
    for ref in totals[1:]:
        summed = summed + ref[...]
    factor = 1.0 / jnp.sum(summed[9:10], axis=1, keepdims=True)
    scaled = summed * factor
    value[...] = scaled[:7]
    rest[...] = jnp.broadcast_to(jnp.sum(scaled[7:9], axis=1, keepdims=True), rest.shape)
    share = one.shape[0]
    cols = one.shape[1] // YS
    wide = 2 * cols // 128
    for y in range(YS):
        total = landed[0, y].astype(f32)
        for z in range(1, ZS):
            total = total + landed[z, y].astype(f32)
        total = total * factor
        last = total[wide * share :]
        last = jnp.concatenate([last[: share - 32, :64], last[:, 64:]], axis=0)
        row = jnp.concatenate(
            [total[n * share : (n + 1) * share] for n in range(wide)] + [last], axis=1
        )
        one[:, y * cols : (y + 1) * cols] = row[:, :cols]
        two[:, y * cols : (y + 1) * cols] = row[:, cols:]


def lookup(ids, table, y):
    count = ids.shape[0]
    local_rows = table.shape[0]
    holders = lax.axis_size(ROWS)
    per_holder = count // holders
    columns = table.shape[1] // YS
    place = jnp.arange(count, dtype=jnp.int32)
    holder = ids // local_rows
    local = ids % local_rows
    earlier = (holder[:, None] == holder[None, :]) & (place[None, :] < place[:, None])
    slot = per_holder * holder + jnp.sum(earlier.astype(jnp.int32), axis=1)
    coded = local + 4096 * place
    asked = jnp.sum(jnp.where(slot[:, None] == place[None, :], coded[:, None], 0), axis=0)
    got = exchange(asked.reshape(holders, per_holder), ROWS).reshape(count)
    found = table[got & 4095]
    where = (got >> 12).astype(bf16)
    found = found.reshape(ZS, YS, CS, per_holder, YS, columns).transpose(0, 4, 2, 1, 3, 5)
    where = jnp.broadcast_to(
        where.reshape(ZS, 1, YS, CS, per_holder, 1).transpose(0, 1, 3, 2, 4, 5),
        (ZS, YS, CS, YS, per_holder, 1),
    )
    sent = jnp.concatenate([found, where], axis=-1).reshape(holders, YS * per_holder, columns + 1)
    back = exchange(sent, ROWS)
    back = back.reshape(holders * YS * per_holder, columns + 1)
    slots = jnp.arange(holders * YS * per_holder, dtype=jnp.int32)
    source = (slots // per_holder % YS + YS - y) % YS
    token = source * count + back[:, columns].astype(jnp.int32)
    one_hot = (token[:, None] == jnp.arange(YS * count, dtype=jnp.int32)[None, :]).astype(bf16)
    rows = back[:, :columns]
    return lax.dot_general(
        one_hot,
        jnp.concatenate([rows, rows, rows, rows], axis=1),
        (((0,), (0,)), ((), ())),
        preferred_element_type=f32,
    ).astype(bf16)


def on_device(
    hidden, rewards, actions, lengths, table, q_one, q_two, t_one, t_two, value_weight, value_bias
):
    prompts, slots, width = hidden.shape
    tokens = prompts * slots
    share, head_cols = q_one.shape
    cols = head_cols // YS
    y = lax.axis_index("y")
    place = jnp.stack([y, lax.axis_index("x"), lax.axis_index("c")]).astype(jnp.int32)
    smem = pl.BlockSpec(memory_space=pltpu.SMEM)
    vmem = pl.BlockSpec(memory_space=VMEM)
    anywhere = pl.BlockSpec(memory_space=pl.ANY)
    limit = pltpu.CompilerParams(vmem_limit_bytes=24 * 1024 * 1024)
    near = functools.partial(pltpu.with_memory_space_constraint, memory_space=VMEM)
    far = functools.partial(pltpu.with_memory_space_constraint, memory_space=pltpu.HBM)

    piece = jax.ShapeDtypeStruct((share, 4 * cols), bf16)
    half = jax.ShapeDtypeStruct((slots, width), bf16)
    *sent, half_a, half_b = pl.pallas_call(
        repack_kernel,
        out_shape=(piece,) * YS + (half, half),
        in_specs=[smem] + [vmem] * 5,
        out_specs=(vmem,) * (YS + 2),
        scratch_shapes=[VMEM((YS, share, 4 * cols), bf16)],
    )(place, q_one, q_two, t_one, t_two, hidden)
    pieces = [sent[0]] + [ahead(sent[s], "y", s) for s in range(1, YS)]
    pieces = pl.pallas_call(
        gather_kernel,
        out_shape=jax.ShapeDtypeStruct((YS, share, 4 * cols), bf16),
        in_specs=[smem] + [vmem] * YS,
        out_specs=vmem,
    )(place, *pieces)
    weights = lax.all_gather(pieces.reshape(YS * share, 4 * cols), ("z", "c"), axis=0, tiled=True)
    weights = weights.reshape(XS, width, 4 * cols)
    a_steps = [ahead(half_a, "x", s) for s in range(1, XS)]
    b_steps = [ahead(half_b, "y", s) for s in range(1, YS)]
    a_part = jnp.stack([half_a] + a_steps)
    b_part = jnp.stack([half_b] + b_steps)
    a_parts = [a_part] + [ahead(a_part, "y", s) for s in range(1, YS)]
    b_parts = [b_part] + [ahead(b_part, "x", s) for s in range(1, XS)]
    embed = lookup(actions.reshape(tokens), table, y)

    value_part = jnp.dot(
        hidden.reshape(tokens, width), value_weight, preferred_element_type=f32
    )
    extras = jnp.concatenate(
        [
            jnp.zeros((4, tokens), f32),
            value_part[None],
            rewards.reshape(1, tokens),
            jnp.repeat(lengths.astype(f32), slots)[None],
            jnp.zeros((1, tokens), f32),
        ]
    )
    group = YS * tokens
    pre, states, said = pl.pallas_call(
        forward_kernel,
        out_shape=(
            pltpu.HBM((group, 512), f32),
            pltpu.HBM((XS, group, width), bf16),
            jax.ShapeDtypeStruct((YS * XS, YS, 8, tokens), f32),
        ),
        in_specs=[smem] + [vmem] * (YS + XS) + [anywhere, anywhere, vmem],
        out_specs=(anywhere, anywhere, vmem),
        scratch_shapes=[
            VMEM((group, 4 * cols), f32),
            VMEM((XS, group, width), bf16),
            VMEM((group, 4 * cols), bf16),
            VMEM((XS, width, 4 * cols), bf16),
            pltpu.SemaphoreType.DMA((XS,)),
            pltpu.SemaphoreType.DMA((XS, YS, 2)),
            pltpu.SemaphoreType.DMA((3,)),
        ],
        compiler_params=limit,
        cost_estimate=pl.CostEstimate(
            flops=2 * group * XS * width * 4 * cols, bytes_accessed=12 << 20, transcendentals=0
        ),
    )(place, *map(near, a_parts), *map(near, b_parts), far(weights), far(embed), extras)

    said = exchange(said, ("y", "x")).reshape(YS, XS, YS, 8, tokens)
    packed = (ZS, YS, 3 * share + 32, 128)
    keep, send, small, value = pl.pallas_call(
        backward_kernel,
        out_shape=(
            VMEM(packed, f32),
            VMEM(packed, bf16),
            jax.ShapeDtypeStruct((8, tokens), f32),
            jax.ShapeDtypeStruct((8, width), f32),
        ),
        in_specs=[smem, smem, vmem] + [anywhere] * 3,
        out_specs=(vmem, vmem, vmem, vmem),
        scratch_shapes=[
            VMEM((group, 512), f32),
            VMEM((group, 512), bf16),
            VMEM((XS, group, width), bf16),
            VMEM((group, 512), bf16),
            VMEM((width, 512), f32),
            pltpu.SemaphoreType.DMA((XS,)),
            pltpu.SemaphoreType.DMA((2,)),
        ],
        compiler_params=limit,
        cost_estimate=pl.CostEstimate(
            flops=2 * group * XS * width * 512, bytes_accessed=12 << 20, transcendentals=0
        ),
    )(place, value_bias, near(said), far(pre), far(embed), far(states))
    terms = (keep + ahead(send, "c", 1).astype(f32)).astype(bf16)
    landed = exchange(terms.reshape(ZS * YS, *packed[2:]), ("z", "y")).reshape(packed)

    value = jnp.sum(value[:3], axis=0).reshape(ZS // XS, CS, YS, share)
    value = value.transpose(0, 2, 1, 3).reshape(width)
    totals = jnp.concatenate([value, small[:3].reshape(-1)])
    totals = sum_over(totals.reshape(-1, tokens), "c")
    totals = [totals] + [ahead(totals, "z", s) for s in range(1, ZS)]
    grad_one, grad_two, grad_value, rest = pl.pallas_call(
        finish_kernel,
        out_shape=(
            jax.ShapeDtypeStruct((share, head_cols), f32),
            jax.ShapeDtypeStruct((share, head_cols), f32),
            jax.ShapeDtypeStruct((width // tokens, tokens), f32),
            jax.ShapeDtypeStruct((2, tokens), f32),
        ),
        in_specs=[vmem] * (ZS + 1),
        out_specs=(vmem, vmem, vmem, vmem),
    )(*map(near, totals), near(landed))

    new_one = (
        (1.0 - polyak_rate) * t_one.astype(f32) + polyak_rate * q_one.astype(f32)
    ).astype(bf16)
    new_two = (
        (1.0 - polyak_rate) * t_two.astype(f32) + polyak_rate * q_two.astype(f32)
    ).astype(bf16)
    return (
        rest[1, 0],
        grad_one,
        grad_two,
        grad_value.reshape(width),
        rest[0, :1],
        new_one,
        new_two,
    )


def solution(mesh):
    fine = Mesh(mesh.devices.reshape(ZS, YS, CS, XS), ("z", "y", "c", "x"))
    in_specs = (
        P(ROWS, None, "x"),
        P(ROWS, None),
        P(ROWS, None),
        P(ROWS),
        P(ROWS, "x"),
        P(ROWS, "x"),
        P(ROWS, "x"),
        P(ROWS, "x"),
        P(ROWS, "x"),
        P("x"),
        P(),
    )
    out_specs = (P(), P(ROWS, "x"), P(ROWS, "x"), P("x"), P(), P(ROWS, "x"), P(ROWS, "x"))

    return jax.shard_map(
        on_device, mesh=fine, in_specs=in_specs, out_specs=out_specs, check_vma=False
    )
```

```python
import functools

import jax
import jax.numpy as jnp
from jax import lax
from jax.experimental import pallas as pl
from jax.experimental.pallas import tpu as pltpu
from jax.sharding import Mesh
from jax.sharding import PartitionSpec as P


discount = 0.99
expectile = 0.7
polyak_rate = 0.005

ZS, YS, CS, XS = 8, 4, 2, 4
ROWS = ("z", "y", "c")
f32 = jnp.float32
bf16 = jnp.bfloat16
VMEM = pltpu.VMEM
root = 0.7978845608028654
cubic = 0.044715


def exchange(pieces, axes):
    return lax.all_to_all(pieces, axes, split_axis=0, concat_axis=0, tiled=True)


def ahead(a, axis, steps):
    n = lax.axis_size(axis)
    return lax.ppermute(a, axis, tuple(((i + steps) % n, i) for i in range(n)))


def sum_over(a, axis):
    n = lax.axis_size(axis)
    return sum([ahead(a, axis, s) for s in range(1, n)], a)


def split_thrice(a):
    first = a.astype(bf16)
    rest = a - first.astype(f32)
    second = rest.astype(bf16)
    third = (rest - second.astype(f32)).astype(bf16)
    return (first, second, third)


def repack_kernel(place, one, two, three, four, hidden, *outs):
    sent, half_a, half_b, out = outs[:YS], *outs[YS:]
    cols = out.shape[2] // 4
    share = one.shape[0]
    for h, ref in enumerate((one, two, three, four)):
        for y in range(YS):
            out[y, :, h * cols : (h + 1) * cols] = ref[:, y * cols : (y + 1) * cols]
    for r in range(YS):
        sent[r][...] = out[lax.rem(place[0] + YS - r, YS)]
    for half, ref in enumerate((half_a, half_b)):
        for z2 in range(ZS // XS):
            for y in range(YS):
                for c in range(CS):
                    old = ((z2 * YS + y) * CS + c) * share
                    new = ((z2 * CS + c) * YS + y) * share
                    ref[:, new : new + share] = hidden[half, :, old : old + share]


def gather_kernel(place, *refs):
    for r in range(YS):
        refs[YS][lax.rem(place[0] + r, YS)] = refs[r][...]


def forward_kernel(place, *refs):
    a_refs, b_refs = refs[:YS], refs[YS : YS + XS]
    weights, pre, held, sems = refs[YS + XS :]
    x = place[1]
    heads_width = weights.shape[2]
    half = pre.shape[0] // 2
    whole = heads_width // 256

    def loads(n):
        at = pl.ds(pl.multiple_of(n * 256, 256), 256) if n < whole else pl.ds(n * 256, 128)
        to = 256 if n < whole else 128
        return [
            pltpu.make_async_copy(
                weights.at[lax.rem(x + xr, XS), :, at], held.at[n, xr, :, :to], sems.at[n, xr]
            )
            for xr in range(XS)
        ]

    for n in range(whole + 1):
        for copy in loads(n):
            copy.start()

    def columns(n, at, wide):
        total_a = total_b = None
        for xr in range(XS):
            block = held[n, xr, :, :wide]
            states_a = jnp.concatenate([a_refs[r][xr] for r in range(YS)], axis=0)
            states_b = b_refs[xr][...].reshape(half, states_a.shape[1])
            part_a = jnp.dot(states_a, block, preferred_element_type=f32)
            part_b = jnp.dot(states_b, block, preferred_element_type=f32)
            total_a = part_a if xr == 0 else total_a + part_a
            total_b = part_b if xr == 0 else total_b + part_b
        pre[:half, at] = total_a
        pre[half:, at] = total_b

    @pl.loop(0, whole)
    def _(n):
        for xr in range(XS):
            pltpu.make_async_copy(
                weights.at[xr, :, :256], held.at[n, xr], sems.at[n, xr]
            ).wait()
        columns(n, pl.ds(pl.multiple_of(n * 256, 256), 256), 256)

    for copy in loads(whole):
        copy.wait()
    columns(whole, slice(whole * 256, heads_width), heads_width - whole * 256)


def score_kernel(place, pre, back, extras, said, kept, embed):
    y = place[0]
    heads_width = pre.shape[1]
    cols = heads_width // 4
    group = pre.shape[0]
    slot_count = group // (2 * YS)
    slots = lax.broadcasted_iota(jnp.int32, (group, 1), 0)
    source = lax.rem(lax.rem(lax.div(slots, 2), YS) + YS - y, YS)
    spot = back[:, cols : cols + 1].astype(f32).astype(jnp.int32)
    late = (spot >= slot_count).astype(jnp.int32)
    token = late * (group // 2) + source * slot_count + spot - late * slot_count
    one_hot = token == lax.broadcasted_iota(jnp.int32, (group, group), 1)
    rows = lax.dot_general(
        one_hot.astype(f32).astype(bf16),
        back[:, :cols],
        (((0,), (0,)), ((), ())),
        preferred_element_type=f32,
    ).astype(bf16)
    for h in range(4):
        embed[:, h * cols : (h + 1) * cols] = rows
    kept[...] = embed[:, : kept.shape[1]]

    @pl.loop(0, YS)
    def _(r):
        total = extras[...]
        low = pl.ds(pl.multiple_of(r * slot_count, slot_count), slot_count)
        high = pl.ds(pl.multiple_of(group // 2 + r * slot_count, slot_count), slot_count)
        for n in range(heads_width // 128):
            lanes = slice(n * 128, (n + 1) * 128)
            p = jnp.concatenate([pre[low, lanes], pre[high, lanes]], axis=0)
            e = jnp.concatenate([embed[low, lanes], embed[high, lanes]], axis=0)
            g = 0.5 * p * (1.0 + jnp.tanh(root * (p + cubic * (p * p * p))))
            g = g * e.astype(f32)
            lane = lax.broadcasted_iota(jnp.int32, (8, 128), 1) + n * 128
            head = lax.broadcasted_iota(jnp.int32, (8, 128), 0)
            chosen = ((lane >= head * cols) & (lane < (head + 1) * cols)).astype(f32).astype(bf16)
            for piece in split_thrice(g):
                total = total + lax.dot_general(
                    chosen, piece, (((1,), (1,)), ((), ())), preferred_element_type=f32
                )
        for copy in range(YS * XS):
            said[copy, lax.rem(y + r, YS)] = total


def backward_kernel(place, bias, said, pre, embed, *refs):
    a_refs, b_refs = refs[:YS], refs[YS : YS + XS]
    keep, send, small, value, held, grads = refs[YS + XS :]
    y, x, core = place[0], place[1], place[2]
    tokens = said.shape[4]
    slot_count = tokens // 2
    half = YS * slot_count
    width = a_refs[0].shape[2]
    share = width // (ZS // XS * YS * CS)
    cols = width // YS
    both = 2 * cols
    slot = lax.rem(lax.broadcasted_iota(jnp.int32, (1, tokens), 1), tokens // 2).astype(f32)
    row = lax.broadcasted_iota(jnp.int32, (8, tokens), 0)
    value[...] = jnp.zeros_like(value)
    bias_sum = loss_sum = count_sum = jnp.zeros((1, tokens), f32)
    for r in range(YS):
        ya = lax.rem(y + r, YS)
        scores = said[0, 0, ya]
        for i in range(1, YS * XS):
            scores = scores + said[i // XS, i % XS, ya]
        mine = said[ya, 0, 0]
        values = mine[4:5]
        for i in range(1, XS):
            values = values + said[ya, i, 0][4:5]
        values = values + bias[0]
        rewards, length = mine[5:6], mine[6:7]
        valid = slot < length
        following = pltpu.roll(values, tokens - 1, 1)
        target = rewards + discount * jnp.where(slot + 1.0 < length, following, 0.0)
        spread = jnp.minimum(scores[2:3], scores[3:4]) - values
        weights = jnp.where(spread < 0.0, 1.0 - expectile, expectile)
        err_one = scores[0:1] - target
        err_two = scores[1:2] - target
        loss_sum = loss_sum + jnp.where(
            valid, err_one * err_one + err_two * err_two + weights * spread * spread, 0.0
        )
        g_one = jnp.where(valid, 2.0 * err_one, 0.0)
        g_two = jnp.where(valid, 2.0 * err_two, 0.0)
        e = jnp.where(valid, -2.0 * weights * spread, 0.0)
        bias_sum = bias_sum + e
        count_sum = count_sum + jnp.where(slot == 0.0, length, 0.0)
        first = e.astype(bf16).astype(f32)
        second = (e - first).astype(bf16).astype(f32)
        third = e - first - second
        thirds = jnp.where(row == 0, first, jnp.where(row == 1, second, third))
        thirds = jnp.where(row < 3, thirds, 0.0).astype(bf16)
        value[...] = (
            value[...]
            + jnp.dot(thirds[:, :slot_count], a_refs[r][0], preferred_element_type=f32)
            + jnp.dot(thirds[:, slot_count:], b_refs[0][r], preferred_element_type=f32)
        )
        upright = jnp.transpose(jnp.where(row == 0, g_one, jnp.where(row == 1, g_two, 0.0)))
        for part in range(2):
            left = upright[part * slot_count : (part + 1) * slot_count, 0:1]
            right = upright[part * slot_count : (part + 1) * slot_count, 1:2]
            at = part * half + r * slot_count
            rows = slice(at, at + slot_count)
            for n in range(held.shape[1] // 128):
                lanes = slice(n * 128, (n + 1) * 128)
                lane = lax.broadcasted_iota(jnp.int32, (slot_count, 128), 1) + n * 128
                g = jnp.where(lane < cols, left, jnp.where(lane < both, right, 0.0))
                p = pre[rows, lanes]
                t = jnp.tanh(root * (p + cubic * (p * p * p)))
                steep = 0.5 * (1.0 + t) + 0.5 * p * (1.0 - t * t) * (
                    root * (1.0 + 3.0 * cubic * (p * p))
                )
                held[rows, lanes] = (g * embed[rows, lanes].astype(f32) * steep).astype(bf16)
    small[...] = jnp.where(
        row == 0, bias_sum, jnp.where(row == 1, loss_sum, jnp.where(row == 2, count_sum, 0.0))
    )

    def against(xr, states_b):
        states_a = jnp.concatenate([ref[xr] for ref in a_refs], axis=0)
        xa = lax.rem(x + xr, XS)
        for n in range(held.shape[1] // 256):
            lanes = slice(n * 256, (n + 1) * 256)
            grads[:, lanes] = lax.dot_general(
                states_a, held[:half, lanes], (((0,), (0,)), ((), ())), preferred_element_type=f32
            ) + lax.dot_general(
                states_b, held[half:, lanes], (((0,), (0,)), ((), ())), preferred_element_type=f32
            )
        for z2 in range(ZS // XS):
            for yy in range(YS):
                to = xa * (ZS // XS) + z2
                low = (z2 * CS * YS + yy) * share
                high = low + YS * share
                for n in range(both // 128):
                    lanes = slice(n * 128, (n + 1) * 128)
                    rows = slice(n * share, (n + 1) * share)
                    first, second = grads[low : low + share, lanes], grads[high : high + share, lanes]
                    keep[to, yy, rows] = jnp.where(core == 0, first, second)
                    send[to, yy, rows] = jnp.where(core == 0, second, first).astype(bf16)
                lanes = slice(both // 128 * 128, both)
                rows = slice(both // 128 * share, None)
                first, second = grads[low : low + share, lanes], grads[high : high + share, lanes]
                mine = jnp.where(core == 0, first, second)
                theirs = jnp.where(core == 0, second, first)
                keep[to, yy, rows] = jnp.concatenate([mine[:32], mine[share - 32 :]], axis=1)
                send[to, yy, rows] = jnp.concatenate(
                    [theirs[:32], theirs[share - 32 :]], axis=1
                ).astype(bf16)

    for xr in range(XS):
        against(xr, b_refs[xr][...].reshape(half, width))


def finish_kernel(*refs):
    totals, landed, one, two, value, rest = refs[:ZS], *refs[ZS:]
    summed = totals[0][...]
    for ref in totals[1:]:
        summed = summed + ref[...]
    factor = 1.0 / jnp.sum(summed[9:10], axis=1, keepdims=True)
    scaled = summed * factor
    value[...] = scaled[:7]
    rest[...] = jnp.broadcast_to(jnp.sum(scaled[7:9], axis=1, keepdims=True), rest.shape)
    share = one.shape[0]
    cols = one.shape[1] // YS
    wide = 2 * cols // 128
    for y in range(YS):
        total = landed[0, y].astype(f32)
        for z in range(1, ZS):
            total = total + landed[z, y].astype(f32)
        total = total * factor
        last = total[wide * share :]
        last = jnp.concatenate([last[: share - 32, :64], last[:, 64:]], axis=0)
        row = jnp.concatenate(
            [total[n * share : (n + 1) * share] for n in range(wide)] + [last], axis=1
        )
        one[:, y * cols : (y + 1) * cols] = row[:, :cols]
        two[:, y * cols : (y + 1) * cols] = row[:, cols:]


def lookup(ids, table):
    count = ids.shape[0]
    local_rows = table.shape[0]
    holders = lax.axis_size(ROWS)
    per_holder = count // holders
    columns = table.shape[1] // YS
    place = jnp.arange(count, dtype=jnp.int32)
    holder = ids // local_rows
    local = ids % local_rows
    earlier = (holder[:, None] == holder[None, :]) & (place[None, :] < place[:, None])
    slot = per_holder * holder + jnp.sum(earlier.astype(jnp.int32), axis=1)
    coded = local + 4096 * place
    asked = jnp.sum(jnp.where(slot[:, None] == place[None, :], coded[:, None], 0), axis=0)
    got = exchange(asked.reshape(holders, per_holder), ROWS).reshape(count)
    found = table[got & 4095]
    where = (got >> 12).astype(bf16)
    found = found.reshape(ZS, YS, CS, per_holder, YS, columns).transpose(0, 4, 2, 1, 3, 5)
    where = jnp.broadcast_to(
        where.reshape(ZS, 1, YS, CS, per_holder, 1).transpose(0, 1, 3, 2, 4, 5),
        (ZS, YS, CS, YS, per_holder, 1),
    )
    sent = jnp.concatenate([found, where], axis=-1).reshape(holders, YS * per_holder, columns + 1)
    back = exchange(sent, ROWS)
    return back.reshape(holders * YS * per_holder, columns + 1)


def on_device(
    hidden, rewards, actions, lengths, table, q_one, q_two, t_one, t_two, value_weight, value_bias
):
    prompts, slots, width = hidden.shape
    tokens = prompts * slots
    share, head_cols = q_one.shape
    cols = head_cols // YS
    y = lax.axis_index("y")
    place = jnp.stack([y, lax.axis_index("x"), lax.axis_index("c")]).astype(jnp.int32)
    smem = pl.BlockSpec(memory_space=pltpu.SMEM)
    vmem = pl.BlockSpec(memory_space=VMEM)
    anywhere = pl.BlockSpec(memory_space=pl.ANY)
    limit = pltpu.CompilerParams(vmem_limit_bytes=24 * 1024 * 1024)
    near = functools.partial(pltpu.with_memory_space_constraint, memory_space=VMEM)
    far = functools.partial(pltpu.with_memory_space_constraint, memory_space=pltpu.HBM)

    piece = jax.ShapeDtypeStruct((share, 4 * cols), bf16)
    half = jax.ShapeDtypeStruct((slots, width), bf16)
    *sent, half_a, half_b = pl.pallas_call(
        repack_kernel,
        out_shape=(piece,) * YS + (half, half),
        in_specs=[smem] + [vmem] * 5,
        out_specs=(vmem,) * (YS + 2),
        scratch_shapes=[VMEM((YS, share, 4 * cols), bf16)],
    )(place, q_one, q_two, t_one, t_two, hidden)
    pieces = [sent[0]] + [ahead(sent[s], "y", s) for s in range(1, YS)]
    pieces = pl.pallas_call(
        gather_kernel,
        out_shape=jax.ShapeDtypeStruct((YS, share, 4 * cols), bf16),
        in_specs=[smem] + [vmem] * YS,
        out_specs=vmem,
    )(place, *pieces)
    weights = lax.all_gather(pieces.reshape(YS * share, 4 * cols), ("z", "c"), axis=0, tiled=True)
    weights = weights.reshape(XS, width, 4 * cols)
    a_steps = [ahead(half_a, "x", s) for s in range(1, XS)]
    b_steps = [ahead(half_b, "y", s) for s in range(1, YS)]
    a_part = jnp.stack([half_a] + a_steps)
    b_part = jnp.stack([half_b] + b_steps)
    a_parts = [a_part] + [ahead(a_part, "y", s) for s in range(1, YS)]
    b_parts = [b_part] + [ahead(b_part, "x", s) for s in range(1, XS)]
    back = lookup(actions.reshape(tokens), table)

    value_part = jnp.dot(
        hidden.reshape(tokens, width), value_weight, preferred_element_type=f32
    )
    extras = jnp.concatenate(
        [
            jnp.zeros((4, tokens), f32),
            value_part[None],
            rewards.reshape(1, tokens),
            jnp.repeat(lengths.astype(f32), slots)[None],
            jnp.zeros((1, tokens), f32),
        ]
    )
    group = YS * tokens
    pre = pl.pallas_call(
        forward_kernel,
        out_shape=jax.ShapeDtypeStruct((group, 4 * cols), f32),
        in_specs=[smem] + [vmem] * (YS + XS) + [anywhere],
        out_specs=vmem,
        scratch_shapes=[
            VMEM((4 * cols // 256 + 1, XS, width, 256), bf16),
            pltpu.SemaphoreType.DMA((4 * cols // 256 + 1, XS)),
        ],
        compiler_params=limit,
        cost_estimate=pl.CostEstimate(
            flops=2 * group * XS * width * 4 * cols, bytes_accessed=12 << 20, transcendentals=0
        ),
    )(place, *a_parts, *b_parts, far(weights))
    said, embed = pl.pallas_call(
        score_kernel,
        out_shape=(
            jax.ShapeDtypeStruct((YS * XS, YS, 8, tokens), f32),
            jax.ShapeDtypeStruct((group, 512), bf16),
        ),
        in_specs=[smem] + [vmem] * 3,
        out_specs=(vmem, vmem),
        scratch_shapes=[VMEM((group, 4 * cols), bf16)],
        compiler_params=limit,
    )(place, pre, back, extras)

    said = exchange(said, ("y", "x")).reshape(YS, XS, YS, 8, tokens)
    packed = (ZS, YS, 3 * share + 32, 128)
    keep, send, small, value = pl.pallas_call(
        backward_kernel,
        out_shape=(
            VMEM(packed, f32),
            VMEM(packed, bf16),
            jax.ShapeDtypeStruct((8, tokens), f32),
            jax.ShapeDtypeStruct((8, width), f32),
        ),
        in_specs=[smem, smem] + [vmem] * (3 + YS + XS),
        out_specs=(vmem, vmem, vmem, vmem),
        scratch_shapes=[VMEM((group, 512), bf16), VMEM((width, 512), f32)],
        compiler_params=limit,
        cost_estimate=pl.CostEstimate(
            flops=2 * group * XS * width * 512, bytes_accessed=12 << 20, transcendentals=0
        ),
    )(place, value_bias, near(said), pre, embed, *a_parts, *b_parts)
    terms = (keep + ahead(send, "c", 1).astype(f32)).astype(bf16)
    landed = exchange(terms.reshape(ZS * YS, *packed[2:]), ("z", "y")).reshape(packed)

    value = jnp.sum(value[:3], axis=0).reshape(ZS // XS, CS, YS, share)
    value = value.transpose(0, 2, 1, 3).reshape(width)
    totals = jnp.concatenate([value, small[:3].reshape(-1)])
    totals = sum_over(totals.reshape(-1, tokens), "c")
    totals = [totals] + [ahead(totals, "z", s) for s in range(1, ZS)]
    grad_one, grad_two, grad_value, rest = pl.pallas_call(
        finish_kernel,
        out_shape=(
            jax.ShapeDtypeStruct((share, head_cols), f32),
            jax.ShapeDtypeStruct((share, head_cols), f32),
            jax.ShapeDtypeStruct((width // tokens, tokens), f32),
            jax.ShapeDtypeStruct((2, tokens), f32),
        ),
        in_specs=[vmem] * (ZS + 1),
        out_specs=(vmem, vmem, vmem, vmem),
    )(*map(near, totals), near(landed))

    new_one = (
        (1.0 - polyak_rate) * t_one.astype(f32) + polyak_rate * q_one.astype(f32)
    ).astype(bf16)
    new_two = (
        (1.0 - polyak_rate) * t_two.astype(f32) + polyak_rate * q_two.astype(f32)
    ).astype(bf16)
    return (
        rest[1, 0],
        grad_one,
        grad_two,
        grad_value.reshape(width),
        rest[0, :1],
        new_one,
        new_two,
    )


def solution(mesh):
    fine = Mesh(mesh.devices.reshape(ZS, YS, CS, XS), ("z", "y", "c", "x"))
    in_specs = (
        P(ROWS, None, "x"),
        P(ROWS, None),
        P(ROWS, None),
        P(ROWS),
        P(ROWS, "x"),
        P(ROWS, "x"),
        P(ROWS, "x"),
        P(ROWS, "x"),
        P(ROWS, "x"),
        P("x"),
        P(),
    )
    out_specs = (P(), P(ROWS, "x"), P(ROWS, "x"), P("x"), P(), P(ROWS, "x"), P(ROWS, "x"))

    return jax.shard_map(
        on_device, mesh=fine, in_specs=in_specs, out_specs=out_specs, check_vma=False
    )
```

```python
import functools

import jax
import jax.numpy as jnp
from jax import lax
from jax.experimental import pallas as pl
from jax.experimental.pallas import tpu as pltpu
from jax.sharding import Mesh
from jax.sharding import PartitionSpec as P


discount = 0.99
expectile = 0.7
polyak_rate = 0.005

ZS, YS, CS, XS = 8, 4, 2, 4
ROWS = ("z", "y", "c")
f32 = jnp.float32
bf16 = jnp.bfloat16
VMEM = pltpu.VMEM
root = 0.7978845608028654
cubic = 0.044715


def exchange(pieces, axes):
    return lax.all_to_all(pieces, axes, split_axis=0, concat_axis=0, tiled=True)


def ahead(a, axis, steps):
    n = lax.axis_size(axis)
    return lax.ppermute(a, axis, tuple(((i + steps) % n, i) for i in range(n)))


def sum_over(a, axis):
    n = lax.axis_size(axis)
    return sum([ahead(a, axis, s) for s in range(1, n)], a)


def split_thrice(a):
    first = a.astype(bf16)
    rest = a - first.astype(f32)
    second = rest.astype(bf16)
    third = (rest - second.astype(f32)).astype(bf16)
    return (first, second, third)


def repack_kernel(place, one, two, three, four, hidden, *outs):
    sent, half_a, half_b, out = outs[:YS], *outs[YS:]
    cols = out.shape[2] // 4
    share = one.shape[0]
    for h, ref in enumerate((one, two, three, four)):
        for y in range(YS):
            out[y, :, h * cols : (h + 1) * cols] = ref[:, y * cols : (y + 1) * cols]
    for r in range(YS):
        sent[r][...] = out[lax.rem(place[0] + YS - r, YS)]
    for half, ref in enumerate((half_a, half_b)):
        for z2 in range(ZS // XS):
            for y in range(YS):
                for c in range(CS):
                    old = ((z2 * YS + y) * CS + c) * share
                    new = ((z2 * CS + c) * YS + y) * share
                    ref[:, new : new + share] = hidden[half, :, old : old + share]


def gather_kernel(place, *refs):
    for r in range(YS):
        refs[YS][lax.rem(place[0] + r, YS)] = refs[r][...]


def piece_copies(a_refs, b_refs, states, sems, xr):
    slot_count = a_refs[0].shape[1]
    found = []
    for r in range(YS):
        low = pl.ds(r * slot_count, slot_count)
        high = pl.ds((YS + r) * slot_count, slot_count)
        for part, (source, to) in enumerate(((a_refs[r].at[xr], low), (b_refs[xr].at[r], high))):
            found.append(pltpu.make_async_copy(source, states.at[xr, to], sems.at[xr, r, part]))
    return found


def forward_kernel(place, *refs):
    a_refs, b_refs = refs[:YS], refs[YS : YS + XS]
    weights, pre, states, held, sems, part_sems = refs[YS + XS :]
    x = place[1]
    heads_width = weights.shape[2]
    whole = heads_width // 256

    def loads(n):
        at = pl.ds(pl.multiple_of(n * 256, 256), 256) if n < whole else pl.ds(n * 256, 128)
        to = 256 if n < whole else 128
        return [
            pltpu.make_async_copy(
                weights.at[lax.rem(x + xr, XS), :, at], held.at[n, xr, :, :to], sems.at[n, xr]
            )
            for xr in range(XS)
        ]

    moves = [
        copy for xr in range(XS) for copy in piece_copies(a_refs, b_refs, states, part_sems, xr)
    ]
    for copy in moves + [copy for n in range(whole + 1) for copy in loads(n)]:
        copy.start()
    for copy in moves:
        copy.wait()

    def columns(n, at, wide):
        total = None
        for xr in range(XS):
            part = jnp.dot(states[xr], held[n, xr, :, :wide], preferred_element_type=f32)
            total = part if xr == 0 else total + part
        pre[:, at] = total

    @pl.loop(0, whole)
    def _(n):
        for xr in range(XS):
            pltpu.make_async_copy(
                weights.at[xr, :, :256], held.at[n, xr], sems.at[n, xr]
            ).wait()
        columns(n, pl.ds(pl.multiple_of(n * 256, 256), 256), 256)

    for copy in loads(whole):
        copy.wait()
    columns(whole, slice(whole * 256, heads_width), heads_width - whole * 256)


def score_kernel(place, pre, back, extras, said, kept, embed, sem):
    y = place[0]
    heads_width = pre.shape[1]
    cols = heads_width // 4
    group = pre.shape[0]
    slot_count = group // (2 * YS)
    slots = lax.broadcasted_iota(jnp.int32, (group, 1), 0)
    source = lax.rem(lax.rem(lax.div(slots, 2), YS) + YS - y, YS)
    spot = back[:, cols : cols + 1].astype(f32).astype(jnp.int32)
    late = (spot >= slot_count).astype(jnp.int32)
    token = late * (group // 2) + source * slot_count + spot - late * slot_count
    one_hot = token == lax.broadcasted_iota(jnp.int32, (group, group), 1)
    rows = lax.dot_general(
        one_hot.astype(f32).astype(bf16),
        back[:, :cols],
        (((0,), (0,)), ((), ())),
        preferred_element_type=f32,
    ).astype(bf16)
    for h in range(4):
        embed[:, h * cols : (h + 1) * cols] = rows
    keep = pltpu.make_async_copy(embed.at[:, : kept.shape[1]], kept, sem)
    keep.start()

    @pl.loop(0, YS)
    def _(r):
        total = extras[...]
        low = pl.ds(pl.multiple_of(r * slot_count, slot_count), slot_count)
        high = pl.ds(pl.multiple_of(group // 2 + r * slot_count, slot_count), slot_count)
        for n in range(heads_width // 128):
            lanes = slice(n * 128, (n + 1) * 128)
            p = jnp.concatenate([pre[low, lanes], pre[high, lanes]], axis=0)
            e = jnp.concatenate([embed[low, lanes], embed[high, lanes]], axis=0)
            g = 0.5 * p * (1.0 + jnp.tanh(root * (p + cubic * (p * p * p))))
            g = g * e.astype(f32)
            lane = lax.broadcasted_iota(jnp.int32, (8, 128), 1) + n * 128
            head = lax.broadcasted_iota(jnp.int32, (8, 128), 0)
            chosen = ((lane >= head * cols) & (lane < (head + 1) * cols)).astype(f32).astype(bf16)
            for piece in split_thrice(g):
                total = total + lax.dot_general(
                    chosen, piece, (((1,), (1,)), ((), ())), preferred_element_type=f32
                )
        for copy in range(YS * XS):
            said[copy, lax.rem(y + r, YS)] = total

    keep.wait()


def backward_kernel(place, bias, said, pre, embed_in, *refs):
    a_refs, b_refs = refs[:YS], refs[YS : YS + XS]
    keep, send, small, value = refs[YS + XS : YS + XS + 4]
    states, embed, held, grads, sems, more = refs[YS + XS + 4 :]
    fetch = pltpu.make_async_copy(embed_in, embed, more)
    fetch.start()
    loads = [piece_copies(a_refs, b_refs, states, sems, xr) for xr in range(XS)]
    for load in sum(loads, []):
        load.start()
    y, x, core = place[0], place[1], place[2]
    tokens = said.shape[4]
    slot_count = tokens // 2
    half = YS * slot_count
    width = states.shape[2]
    share = width // (ZS // XS * YS * CS)
    cols = width // YS
    both = 2 * cols
    slot = lax.rem(lax.broadcasted_iota(jnp.int32, (1, tokens), 1), tokens // 2).astype(f32)
    row = lax.broadcasted_iota(jnp.int32, (8, tokens), 0)
    bias_sum = loss_sum = count_sum = jnp.zeros((1, tokens), f32)
    parts = []
    for r in range(YS):
        ya = lax.rem(y + r, YS)
        scores = said[0, 0, ya]
        for i in range(1, YS * XS):
            scores = scores + said[i // XS, i % XS, ya]
        mine = said[ya, 0, 0]
        values = mine[4:5]
        for i in range(1, XS):
            values = values + said[ya, i, 0][4:5]
        values = values + bias[0]
        rewards, length = mine[5:6], mine[6:7]
        valid = slot < length
        following = pltpu.roll(values, tokens - 1, 1)
        target = rewards + discount * jnp.where(slot + 1.0 < length, following, 0.0)
        spread = jnp.minimum(scores[2:3], scores[3:4]) - values
        weights = jnp.where(spread < 0.0, 1.0 - expectile, expectile)
        err_one = scores[0:1] - target
        err_two = scores[1:2] - target
        loss_sum = loss_sum + jnp.where(
            valid, err_one * err_one + err_two * err_two + weights * spread * spread, 0.0
        )
        g_one = jnp.where(valid, 2.0 * err_one, 0.0)
        g_two = jnp.where(valid, 2.0 * err_two, 0.0)
        e = jnp.where(valid, -2.0 * weights * spread, 0.0)
        bias_sum = bias_sum + e
        count_sum = count_sum + jnp.where(slot == 0.0, length, 0.0)
        first = e.astype(bf16).astype(f32)
        second = (e - first).astype(bf16).astype(f32)
        third = e - first - second
        thirds = jnp.where(row == 0, first, jnp.where(row == 1, second, third))
        thirds = jnp.where(row < 3, thirds, 0.0).astype(bf16)
        parts.append(thirds)
        upright = jnp.transpose(jnp.where(row == 0, g_one, jnp.where(row == 1, g_two, 0.0)))
        if r == 0:
            fetch.wait()
        for part in range(2):
            left = upright[part * slot_count : (part + 1) * slot_count, 0:1]
            right = upright[part * slot_count : (part + 1) * slot_count, 1:2]
            at = part * half + r * slot_count
            rows = slice(at, at + slot_count)
            for n in range(held.shape[1] // 128):
                lanes = slice(n * 128, (n + 1) * 128)
                lane = lax.broadcasted_iota(jnp.int32, (slot_count, 128), 1) + n * 128
                g = jnp.where(lane < cols, left, jnp.where(lane < both, right, 0.0))
                p = pre[rows, lanes]
                t = jnp.tanh(root * (p + cubic * (p * p * p)))
                steep = 0.5 * (1.0 + t) + 0.5 * p * (1.0 - t * t) * (
                    root * (1.0 + 3.0 * cubic * (p * p))
                )
                held[rows, lanes] = (g * embed[rows, lanes].astype(f32) * steep).astype(bf16)
    small[...] = jnp.where(
        row == 0, bias_sum, jnp.where(row == 1, loss_sum, jnp.where(row == 2, count_sum, 0.0))
    )

    def against(xr):
        xa = lax.rem(x + xr, XS)
        for n in range(held.shape[1] // 256):
            lanes = slice(n * 256, (n + 1) * 256)
            grads[:, lanes] = lax.dot_general(
                states[xr], held[:, lanes], (((0,), (0,)), ((), ())), preferred_element_type=f32
            )
        for z2 in range(ZS // XS):
            for yy in range(YS):
                to = xa * (ZS // XS) + z2
                low = (z2 * CS * YS + yy) * share
                high = low + YS * share
                for n in range(both // 128):
                    lanes = slice(n * 128, (n + 1) * 128)
                    rows = slice(n * share, (n + 1) * share)
                    first, second = grads[low : low + share, lanes], grads[high : high + share, lanes]
                    keep[to, yy, rows] = jnp.where(core == 0, first, second)
                    send[to, yy, rows] = jnp.where(core == 0, second, first).astype(bf16)
                lanes = slice(both // 128 * 128, both)
                rows = slice(both // 128 * share, None)
                first, second = grads[low : low + share, lanes], grads[high : high + share, lanes]
                mine = jnp.where(core == 0, first, second)
                theirs = jnp.where(core == 0, second, first)
                keep[to, yy, rows] = jnp.concatenate([mine[:32], mine[share - 32 :]], axis=1)
                send[to, yy, rows] = jnp.concatenate(
                    [theirs[:32], theirs[share - 32 :]], axis=1
                ).astype(bf16)

    for load in loads[0]:
        load.wait()
    total = jnp.zeros((8, width), f32)
    for r, thirds in enumerate(parts):
        for part in range(2):
            at = part * half + r * slot_count
            total = total + jnp.dot(
                thirds[:, part * slot_count : (part + 1) * slot_count],
                states[0, at : at + slot_count],
                preferred_element_type=f32,
            )
    value[...] = total
    against(0)
    for load in sum(loads[1:], []):
        load.wait()

    @pl.loop(1, XS)
    def _(xr):
        against(xr)


def finish_kernel(*refs):
    totals, landed, one, two, value, rest = refs[:ZS], *refs[ZS:]
    summed = totals[0][...]
    for ref in totals[1:]:
        summed = summed + ref[...]
    factor = 1.0 / jnp.sum(summed[9:10], axis=1, keepdims=True)
    scaled = summed * factor
    value[...] = scaled[:7]
    rest[...] = jnp.broadcast_to(jnp.sum(scaled[7:9], axis=1, keepdims=True), rest.shape)
    share = one.shape[0]
    cols = one.shape[1] // YS
    wide = 2 * cols // 128
    for y in range(YS):
        total = landed[0, y].astype(f32)
        for z in range(1, ZS):
            total = total + landed[z, y].astype(f32)
        total = total * factor
        last = total[wide * share :]
        last = jnp.concatenate([last[: share - 32, :64], last[:, 64:]], axis=0)
        row = jnp.concatenate(
            [total[n * share : (n + 1) * share] for n in range(wide)] + [last], axis=1
        )
        one[:, y * cols : (y + 1) * cols] = row[:, :cols]
        two[:, y * cols : (y + 1) * cols] = row[:, cols:]


def lookup(ids, table):
    count = ids.shape[0]
    local_rows = table.shape[0]
    holders = lax.axis_size(ROWS)
    per_holder = count // holders
    columns = table.shape[1] // YS
    place = jnp.arange(count, dtype=jnp.int32)
    holder = ids // local_rows
    local = ids % local_rows
    earlier = (holder[:, None] == holder[None, :]) & (place[None, :] < place[:, None])
    slot = per_holder * holder + jnp.sum(earlier.astype(jnp.int32), axis=1)
    coded = local + 4096 * place
    asked = jnp.sum(jnp.where(slot[:, None] == place[None, :], coded[:, None], 0), axis=0)
    got = exchange(asked.reshape(holders, per_holder), ROWS).reshape(count)
    found = table[got & 4095]
    where = (got >> 12).astype(bf16)
    found = found.reshape(ZS, YS, CS, per_holder, YS, columns).transpose(0, 4, 2, 1, 3, 5)
    where = jnp.broadcast_to(
        where.reshape(ZS, 1, YS, CS, per_holder, 1).transpose(0, 1, 3, 2, 4, 5),
        (ZS, YS, CS, YS, per_holder, 1),
    )
    sent = jnp.concatenate([found, where], axis=-1).reshape(holders, YS * per_holder, columns + 1)
    back = exchange(sent, ROWS)
    return back.reshape(holders * YS * per_holder, columns + 1)


def on_device(
    hidden, rewards, actions, lengths, table, q_one, q_two, t_one, t_two, value_weight, value_bias
):
    prompts, slots, width = hidden.shape
    tokens = prompts * slots
    share, head_cols = q_one.shape
    cols = head_cols // YS
    y = lax.axis_index("y")
    place = jnp.stack([y, lax.axis_index("x"), lax.axis_index("c")]).astype(jnp.int32)
    smem = pl.BlockSpec(memory_space=pltpu.SMEM)
    vmem = pl.BlockSpec(memory_space=VMEM)
    anywhere = pl.BlockSpec(memory_space=pl.ANY)
    limit = pltpu.CompilerParams(vmem_limit_bytes=24 * 1024 * 1024)
    near = functools.partial(pltpu.with_memory_space_constraint, memory_space=VMEM)
    far = functools.partial(pltpu.with_memory_space_constraint, memory_space=pltpu.HBM)

    piece = jax.ShapeDtypeStruct((share, 4 * cols), bf16)
    half = jax.ShapeDtypeStruct((slots, width), bf16)
    *sent, half_a, half_b = pl.pallas_call(
        repack_kernel,
        out_shape=(piece,) * YS + (half, half),
        in_specs=[smem] + [vmem] * 5,
        out_specs=(vmem,) * (YS + 2),
        scratch_shapes=[VMEM((YS, share, 4 * cols), bf16)],
    )(place, q_one, q_two, t_one, t_two, hidden)
    pieces = [sent[0]] + [ahead(sent[s], "y", s) for s in range(1, YS)]
    pieces = pl.pallas_call(
        gather_kernel,
        out_shape=jax.ShapeDtypeStruct((YS, share, 4 * cols), bf16),
        in_specs=[smem] + [vmem] * YS,
        out_specs=vmem,
    )(place, *pieces)
    weights = lax.all_gather(pieces.reshape(YS * share, 4 * cols), ("z", "c"), axis=0, tiled=True)
    weights = weights.reshape(XS, width, 4 * cols)
    a_steps = [ahead(half_a, "x", s) for s in range(1, XS)]
    b_steps = [ahead(half_b, "y", s) for s in range(1, YS)]
    a_part = jnp.stack([half_a] + a_steps)
    b_part = jnp.stack([half_b] + b_steps)
    a_parts = [a_part] + [ahead(a_part, "y", s) for s in range(1, YS)]
    b_parts = [b_part] + [ahead(b_part, "x", s) for s in range(1, XS)]
    back = lookup(actions.reshape(tokens), table)

    value_part = jnp.dot(
        hidden.reshape(tokens, width), value_weight, preferred_element_type=f32
    )
    extras = jnp.concatenate(
        [
            jnp.zeros((4, tokens), f32),
            value_part[None],
            rewards.reshape(1, tokens),
            jnp.repeat(lengths.astype(f32), slots)[None],
            jnp.zeros((1, tokens), f32),
        ]
    )
    group = YS * tokens
    landed_parts = tuple(map(far, (*a_parts, *b_parts)))
    pre = pl.pallas_call(
        forward_kernel,
        out_shape=jax.ShapeDtypeStruct((group, 4 * cols), f32),
        in_specs=[smem] + [anywhere] * (YS + XS + 1),
        out_specs=vmem,
        scratch_shapes=[
            VMEM((XS, group, width), bf16),
            VMEM((4 * cols // 256 + 1, XS, width, 256), bf16),
            pltpu.SemaphoreType.DMA((4 * cols // 256 + 1, XS)),
            pltpu.SemaphoreType.DMA((XS, YS, 2)),
        ],
        compiler_params=limit,
        cost_estimate=pl.CostEstimate(
            flops=2 * group * XS * width * 4 * cols, bytes_accessed=12 << 20, transcendentals=0
        ),
    )(place, *landed_parts, far(weights))
    said, embed = pl.pallas_call(
        score_kernel,
        out_shape=(
            jax.ShapeDtypeStruct((YS * XS, YS, 8, tokens), f32),
            pltpu.HBM((group, 512), bf16),
        ),
        in_specs=[smem] + [vmem] * 3,
        out_specs=(vmem, anywhere),
        scratch_shapes=[VMEM((group, 4 * cols), bf16), pltpu.SemaphoreType.DMA],
        compiler_params=limit,
    )(place, pre, back, extras)

    said = exchange(said, ("y", "x")).reshape(YS, XS, YS, 8, tokens)
    packed = (ZS, YS, 3 * share + 32, 128)
    keep, send, small, value = pl.pallas_call(
        backward_kernel,
        out_shape=(
            VMEM(packed, f32),
            VMEM(packed, bf16),
            jax.ShapeDtypeStruct((8, tokens), f32),
            jax.ShapeDtypeStruct((8, width), f32),
        ),
        in_specs=[smem, smem, vmem, vmem] + [anywhere] * (1 + YS + XS),
        out_specs=(vmem, vmem, vmem, vmem),
        scratch_shapes=[
            VMEM((XS, group, width), bf16),
            VMEM((group, 512), bf16),
            VMEM((group, 512), bf16),
            VMEM((width, 512), f32),
            pltpu.SemaphoreType.DMA((XS, YS, 2)),
            pltpu.SemaphoreType.DMA,
        ],
        compiler_params=limit,
        cost_estimate=pl.CostEstimate(
            flops=2 * group * XS * width * 512, bytes_accessed=12 << 20, transcendentals=0
        ),
    )(place, value_bias, near(said), pre, far(embed), *landed_parts)
    terms = (keep + ahead(send, "c", 1).astype(f32)).astype(bf16)
    landed = exchange(terms.reshape(ZS * YS, *packed[2:]), ("z", "y")).reshape(packed)

    value = jnp.sum(value[:3], axis=0).reshape(ZS // XS, CS, YS, share)
    value = value.transpose(0, 2, 1, 3).reshape(width)
    totals = jnp.concatenate([value, small[:3].reshape(-1)])
    totals = sum_over(totals.reshape(-1, tokens), "c")
    totals = [totals] + [ahead(totals, "z", s) for s in range(1, ZS)]
    grad_one, grad_two, grad_value, rest = pl.pallas_call(
        finish_kernel,
        out_shape=(
            jax.ShapeDtypeStruct((share, head_cols), f32),
            jax.ShapeDtypeStruct((share, head_cols), f32),
            jax.ShapeDtypeStruct((width // tokens, tokens), f32),
            jax.ShapeDtypeStruct((2, tokens), f32),
        ),
        in_specs=[vmem] * (ZS + 1),
        out_specs=(vmem, vmem, vmem, vmem),
    )(*map(near, totals), near(landed))

    new_one = (
        (1.0 - polyak_rate) * t_one.astype(f32) + polyak_rate * q_one.astype(f32)
    ).astype(bf16)
    new_two = (
        (1.0 - polyak_rate) * t_two.astype(f32) + polyak_rate * q_two.astype(f32)
    ).astype(bf16)
    return (
        rest[1, 0],
        grad_one,
        grad_two,
        grad_value.reshape(width),
        rest[0, :1],
        new_one,
        new_two,
    )


def solution(mesh):
    fine = Mesh(mesh.devices.reshape(ZS, YS, CS, XS), ("z", "y", "c", "x"))
    in_specs = (
        P(ROWS, None, "x"),
        P(ROWS, None),
        P(ROWS, None),
        P(ROWS),
        P(ROWS, "x"),
        P(ROWS, "x"),
        P(ROWS, "x"),
        P(ROWS, "x"),
        P(ROWS, "x"),
        P("x"),
        P(),
    )
    out_specs = (P(), P(ROWS, "x"), P(ROWS, "x"), P("x"), P(), P(ROWS, "x"), P(ROWS, "x"))

    return jax.shard_map(
        on_device, mesh=fine, in_specs=in_specs, out_specs=out_specs, check_vma=False
    )
```

```python
import functools

import jax
import jax.numpy as jnp
from jax import lax
from jax.experimental import pallas as pl
from jax.experimental.pallas import tpu as pltpu
from jax.sharding import Mesh
from jax.sharding import PartitionSpec as P


discount = 0.99
expectile = 0.7
polyak_rate = 0.005

ZS, YS, CS, XS = 8, 4, 2, 4
ROWS = ("z", "y", "c")
f32 = jnp.float32
bf16 = jnp.bfloat16
VMEM = pltpu.VMEM
root = 0.7978845608028654
cubic = 0.044715


def exchange(pieces, axes):
    return lax.all_to_all(pieces, axes, split_axis=0, concat_axis=0, tiled=True)


def ahead(a, axis, steps):
    n = lax.axis_size(axis)
    return lax.ppermute(a, axis, tuple(((i + steps) % n, i) for i in range(n)))


def sum_over(a, axis):
    n = lax.axis_size(axis)
    return sum([ahead(a, axis, s) for s in range(1, n)], a)


def split_thrice(a):
    first = a.astype(bf16)
    rest = a - first.astype(f32)
    second = rest.astype(bf16)
    third = (rest - second.astype(f32)).astype(bf16)
    return (first, second, third)


def repack_kernel(place, one, two, three, four, hidden, *outs):
    sent, half_a, half_b, out = outs[:YS], *outs[YS:]
    cols = out.shape[2] // 4
    share = one.shape[0]
    for h, ref in enumerate((one, two, three, four)):
        for y in range(YS):
            out[y, :, h * cols : (h + 1) * cols] = ref[:, y * cols : (y + 1) * cols]
    for r in range(YS):
        sent[r][...] = out[lax.rem(place[0] + YS - r, YS)]
    for half, ref in enumerate((half_a, half_b)):
        for z2 in range(ZS // XS):
            for y in range(YS):
                for c in range(CS):
                    old = ((z2 * YS + y) * CS + c) * share
                    new = ((z2 * CS + c) * YS + y) * share
                    ref[:, new : new + share] = hidden[half, :, old : old + share]


def gather_kernel(place, *refs):
    for r in range(YS):
        refs[YS][lax.rem(place[0] + r, YS)] = refs[r][...]


def piece_copies(a_refs, b_refs, states, sems, xr):
    slot_count = a_refs[0].shape[1]
    found = []
    for r in range(YS):
        low = pl.ds(r * slot_count, slot_count)
        high = pl.ds((YS + r) * slot_count, slot_count)
        for part, (source, to) in enumerate(((a_refs[r].at[xr], low), (b_refs[xr].at[r], high))):
            found.append(pltpu.make_async_copy(source, states.at[xr, to], sems.at[xr, r, part]))
    return found


def forward_kernel(place, *refs):
    a_refs, b_refs = refs[:YS], refs[YS : YS + XS]
    weights, pre, states, held, sems, part_sems = refs[YS + XS :]
    x = place[1]
    heads_width = weights.shape[2]
    whole = heads_width // 256

    def load(xr):
        return pltpu.make_async_copy(weights.at[lax.rem(x + xr, XS)], held.at[xr], sems.at[xr])

    moves = [piece_copies(a_refs, b_refs, states, part_sems, xr) for xr in range(XS)]
    for xr in range(XS):
        for copy in moves[xr]:
            copy.start()
        load(xr).start()

    def columns(xr, first):
        def add(at):
            part = jnp.dot(states[xr], held[xr, :, at], preferred_element_type=f32)
            pre[:, at] = part if first else pre[:, at] + part

        @pl.loop(0, whole)
        def _(n):
            add(pl.ds(pl.multiple_of(n * 256, 256), 256))

        if heads_width > whole * 256:
            add(slice(whole * 256, heads_width))

    for copy in moves[0]:
        copy.wait()
    load(0).wait()
    columns(0, True)
    for copy in sum(moves[1:], []):
        copy.wait()

    @pl.loop(1, XS)
    def _(xr):
        load(xr).wait()
        columns(xr, False)


def score_kernel(place, pre, back, extras, said, kept, embed, sem):
    y = place[0]
    heads_width = pre.shape[1]
    cols = heads_width // 4
    group = pre.shape[0]
    slot_count = group // (2 * YS)
    slots = lax.broadcasted_iota(jnp.int32, (group, 1), 0)
    source = lax.rem(lax.rem(lax.div(slots, 2), YS) + YS - y, YS)
    spot = back[:, cols : cols + 1].astype(f32).astype(jnp.int32)
    late = (spot >= slot_count).astype(jnp.int32)
    token = late * (group // 2) + source * slot_count + spot - late * slot_count
    one_hot = token == lax.broadcasted_iota(jnp.int32, (group, group), 1)
    rows = lax.dot_general(
        one_hot.astype(f32).astype(bf16),
        back[:, :cols],
        (((0,), (0,)), ((), ())),
        preferred_element_type=f32,
    ).astype(bf16)
    for h in range(4):
        embed[:, h * cols : (h + 1) * cols] = rows
    keep = pltpu.make_async_copy(embed.at[:, : kept.shape[1]], kept, sem)
    keep.start()

    @pl.loop(0, YS)
    def _(r):
        total = extras[...]
        low = pl.ds(pl.multiple_of(r * slot_count, slot_count), slot_count)
        high = pl.ds(pl.multiple_of(group // 2 + r * slot_count, slot_count), slot_count)
        for n in range(heads_width // 128):
            lanes = slice(n * 128, (n + 1) * 128)
            p = jnp.concatenate([pre[low, lanes], pre[high, lanes]], axis=0)
            e = jnp.concatenate([embed[low, lanes], embed[high, lanes]], axis=0)
            g = 0.5 * p * (1.0 + jnp.tanh(root * (p + cubic * (p * p * p))))
            g = g * e.astype(f32)
            lane = lax.broadcasted_iota(jnp.int32, (8, 128), 1) + n * 128
            head = lax.broadcasted_iota(jnp.int32, (8, 128), 0)
            chosen = ((lane >= head * cols) & (lane < (head + 1) * cols)).astype(f32).astype(bf16)
            for piece in split_thrice(g):
                total = total + lax.dot_general(
                    chosen, piece, (((1,), (1,)), ((), ())), preferred_element_type=f32
                )
        for copy in range(YS * XS):
            said[copy, lax.rem(y + r, YS)] = total

    keep.wait()


def backward_kernel(place, bias, said, pre, embed_in, *refs):
    a_refs, b_refs = refs[:YS], refs[YS : YS + XS]
    keep, send, small, value = refs[YS + XS : YS + XS + 4]
    states, embed, held, grads, sems, more = refs[YS + XS + 4 :]
    fetch = pltpu.make_async_copy(embed_in, embed, more)
    fetch.start()
    loads = [piece_copies(a_refs, b_refs, states, sems, xr) for xr in range(XS)]
    for load in sum(loads, []):
        load.start()
    y, x, core = place[0], place[1], place[2]
    tokens = said.shape[4]
    slot_count = tokens // 2
    half = YS * slot_count
    width = states.shape[2]
    share = width // (ZS // XS * YS * CS)
    cols = width // YS
    both = 2 * cols
    slot = lax.rem(lax.broadcasted_iota(jnp.int32, (1, tokens), 1), tokens // 2).astype(f32)
    row = lax.broadcasted_iota(jnp.int32, (8, tokens), 0)
    bias_sum = loss_sum = count_sum = jnp.zeros((1, tokens), f32)
    parts = []
    for r in range(YS):
        ya = lax.rem(y + r, YS)
        scores = said[0, 0, ya]
        for i in range(1, YS * XS):
            scores = scores + said[i // XS, i % XS, ya]
        mine = said[ya, 0, 0]
        values = mine[4:5]
        for i in range(1, XS):
            values = values + said[ya, i, 0][4:5]
        values = values + bias[0]
        rewards, length = mine[5:6], mine[6:7]
        valid = slot < length
        following = pltpu.roll(values, tokens - 1, 1)
        target = rewards + discount * jnp.where(slot + 1.0 < length, following, 0.0)
        spread = jnp.minimum(scores[2:3], scores[3:4]) - values
        weights = jnp.where(spread < 0.0, 1.0 - expectile, expectile)
        err_one = scores[0:1] - target
        err_two = scores[1:2] - target
        loss_sum = loss_sum + jnp.where(
            valid, err_one * err_one + err_two * err_two + weights * spread * spread, 0.0
        )
        g_one = jnp.where(valid, 2.0 * err_one, 0.0)
        g_two = jnp.where(valid, 2.0 * err_two, 0.0)
        e = jnp.where(valid, -2.0 * weights * spread, 0.0)
        bias_sum = bias_sum + e
        count_sum = count_sum + jnp.where(slot == 0.0, length, 0.0)
        first = e.astype(bf16).astype(f32)
        second = (e - first).astype(bf16).astype(f32)
        third = e - first - second
        thirds = jnp.where(row == 0, first, jnp.where(row == 1, second, third))
        thirds = jnp.where(row < 3, thirds, 0.0).astype(bf16)
        parts.append(thirds)
        upright = jnp.transpose(jnp.where(row == 0, g_one, jnp.where(row == 1, g_two, 0.0)))
        if r == 0:
            fetch.wait()
        for part in range(2):
            left = upright[part * slot_count : (part + 1) * slot_count, 0:1]
            right = upright[part * slot_count : (part + 1) * slot_count, 1:2]
            at = part * half + r * slot_count
            rows = slice(at, at + slot_count)
            for n in range(held.shape[1] // 128):
                lanes = slice(n * 128, (n + 1) * 128)
                lane = lax.broadcasted_iota(jnp.int32, (slot_count, 128), 1) + n * 128
                g = jnp.where(lane < cols, left, jnp.where(lane < both, right, 0.0))
                p = pre[rows, lanes]
                t = jnp.tanh(root * (p + cubic * (p * p * p)))
                steep = 0.5 * (1.0 + t) + 0.5 * p * (1.0 - t * t) * (
                    root * (1.0 + 3.0 * cubic * (p * p))
                )
                held[rows, lanes] = (g * embed[rows, lanes].astype(f32) * steep).astype(bf16)
    small[...] = jnp.where(
        row == 0, bias_sum, jnp.where(row == 1, loss_sum, jnp.where(row == 2, count_sum, 0.0))
    )

    def against(xr):
        xa = lax.rem(x + xr, XS)
        for n in range(held.shape[1] // 256):
            lanes = slice(n * 256, (n + 1) * 256)
            grads[:, lanes] = lax.dot_general(
                states[xr], held[:, lanes], (((0,), (0,)), ((), ())), preferred_element_type=f32
            )
        for z2 in range(ZS // XS):
            for yy in range(YS):
                to = xa * (ZS // XS) + z2
                low = (z2 * CS * YS + yy) * share
                high = low + YS * share
                for n in range(both // 128):
                    lanes = slice(n * 128, (n + 1) * 128)
                    rows = slice(n * share, (n + 1) * share)
                    first, second = grads[low : low + share, lanes], grads[high : high + share, lanes]
                    keep[to, yy, rows] = jnp.where(core == 0, first, second)
                    send[to, yy, rows] = jnp.where(core == 0, second, first).astype(bf16)
                lanes = slice(both // 128 * 128, both)
                rows = slice(both // 128 * share, None)
                first, second = grads[low : low + share, lanes], grads[high : high + share, lanes]
                mine = jnp.where(core == 0, first, second)
                theirs = jnp.where(core == 0, second, first)
                keep[to, yy, rows] = jnp.concatenate([mine[:32], mine[share - 32 :]], axis=1)
                send[to, yy, rows] = jnp.concatenate(
                    [theirs[:32], theirs[share - 32 :]], axis=1
                ).astype(bf16)

    for load in loads[0]:
        load.wait()
    total = jnp.zeros((8, width), f32)
    for r, thirds in enumerate(parts):
        for part in range(2):
            at = part * half + r * slot_count
            total = total + jnp.dot(
                thirds[:, part * slot_count : (part + 1) * slot_count],
                states[0, at : at + slot_count],
                preferred_element_type=f32,
            )
    value[...] = total
    for load in sum(loads[1:], []):
        load.wait()

    @pl.loop(0, XS)
    def _(xr):
        against(xr)


def finish_kernel(*refs):
    totals, landed, one, two, value, rest = refs[:ZS], *refs[ZS:]
    summed = totals[0][...]
    for ref in totals[1:]:
        summed = summed + ref[...]
    factor = 1.0 / jnp.sum(summed[9:10], axis=1, keepdims=True)
    scaled = summed * factor
    value[...] = scaled[:7]
    rest[...] = jnp.broadcast_to(jnp.sum(scaled[7:9], axis=1, keepdims=True), rest.shape)
    share = one.shape[0]
    cols = one.shape[1] // YS
    wide = 2 * cols // 128
    for y in range(YS):
        total = landed[0, y].astype(f32)
        for z in range(1, ZS):
            total = total + landed[z, y].astype(f32)
        total = total * factor
        last = total[wide * share :]
        last = jnp.concatenate([last[: share - 32, :64], last[:, 64:]], axis=0)
        row = jnp.concatenate(
            [total[n * share : (n + 1) * share] for n in range(wide)] + [last], axis=1
        )
        one[:, y * cols : (y + 1) * cols] = row[:, :cols]
        two[:, y * cols : (y + 1) * cols] = row[:, cols:]


def lookup(ids, table):
    count = ids.shape[0]
    local_rows = table.shape[0]
    holders = lax.axis_size(ROWS)
    per_holder = count // holders
    columns = table.shape[1] // YS
    place = jnp.arange(count, dtype=jnp.int32)
    holder = ids // local_rows
    local = ids % local_rows
    earlier = (holder[:, None] == holder[None, :]) & (place[None, :] < place[:, None])
    slot = per_holder * holder + jnp.sum(earlier.astype(jnp.int32), axis=1)
    coded = local + 4096 * place
    asked = jnp.sum(jnp.where(slot[:, None] == place[None, :], coded[:, None], 0), axis=0)
    got = exchange(asked.reshape(holders, per_holder), ROWS).reshape(count)
    found = table[got & 4095]
    where = (got >> 12).astype(bf16)
    found = found.reshape(ZS, YS, CS, per_holder, YS, columns).transpose(0, 4, 2, 1, 3, 5)
    where = jnp.broadcast_to(
        where.reshape(ZS, 1, YS, CS, per_holder, 1).transpose(0, 1, 3, 2, 4, 5),
        (ZS, YS, CS, YS, per_holder, 1),
    )
    sent = jnp.concatenate([found, where], axis=-1).reshape(holders, YS * per_holder, columns + 1)
    back = exchange(sent, ROWS)
    return back.reshape(holders * YS * per_holder, columns + 1)


def on_device(
    hidden, rewards, actions, lengths, table, q_one, q_two, t_one, t_two, value_weight, value_bias
):
    prompts, slots, width = hidden.shape
    tokens = prompts * slots
    share, head_cols = q_one.shape
    cols = head_cols // YS
    y = lax.axis_index("y")
    place = jnp.stack([y, lax.axis_index("x"), lax.axis_index("c")]).astype(jnp.int32)
    smem = pl.BlockSpec(memory_space=pltpu.SMEM)
    vmem = pl.BlockSpec(memory_space=VMEM)
    anywhere = pl.BlockSpec(memory_space=pl.ANY)
    limit = pltpu.CompilerParams(vmem_limit_bytes=24 * 1024 * 1024)
    near = functools.partial(pltpu.with_memory_space_constraint, memory_space=VMEM)
    far = functools.partial(pltpu.with_memory_space_constraint, memory_space=pltpu.HBM)

    piece = jax.ShapeDtypeStruct((share, 4 * cols), bf16)
    half = jax.ShapeDtypeStruct((slots, width), bf16)
    *sent, half_a, half_b = pl.pallas_call(
        repack_kernel,
        out_shape=(piece,) * YS + (half, half),
        in_specs=[smem] + [vmem] * 5,
        out_specs=(vmem,) * (YS + 2),
        scratch_shapes=[VMEM((YS, share, 4 * cols), bf16)],
    )(place, q_one, q_two, t_one, t_two, hidden)
    pieces = [sent[0]] + [ahead(sent[s], "y", s) for s in range(1, YS)]
    pieces = pl.pallas_call(
        gather_kernel,
        out_shape=jax.ShapeDtypeStruct((YS, share, 4 * cols), bf16),
        in_specs=[smem] + [vmem] * YS,
        out_specs=vmem,
    )(place, *pieces)
    weights = lax.all_gather(pieces.reshape(YS * share, 4 * cols), ("z", "c"), axis=0, tiled=True)
    weights = weights.reshape(XS, width, 4 * cols)
    a_steps = [ahead(half_a, "x", s) for s in range(1, XS)]
    b_steps = [ahead(half_b, "y", s) for s in range(1, YS)]
    a_part = jnp.stack([half_a] + a_steps)
    b_part = jnp.stack([half_b] + b_steps)
    a_parts = [a_part] + [ahead(a_part, "y", s) for s in range(1, YS)]
    b_parts = [b_part] + [ahead(b_part, "x", s) for s in range(1, XS)]
    back = lookup(actions.reshape(tokens), table)

    value_part = jnp.dot(
        hidden.reshape(tokens, width), value_weight, preferred_element_type=f32
    )
    extras = jnp.concatenate(
        [
            jnp.zeros((4, tokens), f32),
            value_part[None],
            rewards.reshape(1, tokens),
            jnp.repeat(lengths.astype(f32), slots)[None],
            jnp.zeros((1, tokens), f32),
        ]
    )
    group = YS * tokens
    landed_parts = tuple(map(far, (*a_parts, *b_parts)))
    pre = pl.pallas_call(
        forward_kernel,
        out_shape=jax.ShapeDtypeStruct((group, 4 * cols), f32),
        in_specs=[smem] + [anywhere] * (YS + XS + 1),
        out_specs=vmem,
        scratch_shapes=[
            VMEM((XS, group, width), bf16),
            VMEM((XS, width, 4 * cols), bf16),
            pltpu.SemaphoreType.DMA((XS,)),
            pltpu.SemaphoreType.DMA((XS, YS, 2)),
        ],
        compiler_params=limit,
        cost_estimate=pl.CostEstimate(
            flops=2 * group * XS * width * 4 * cols, bytes_accessed=12 << 20, transcendentals=0
        ),
    )(place, *landed_parts, far(weights))
    said, embed = pl.pallas_call(
        score_kernel,
        out_shape=(
            jax.ShapeDtypeStruct((YS * XS, YS, 8, tokens), f32),
            pltpu.HBM((group, 512), bf16),
        ),
        in_specs=[smem] + [vmem] * 3,
        out_specs=(vmem, anywhere),
        scratch_shapes=[VMEM((group, 4 * cols), bf16), pltpu.SemaphoreType.DMA],
        compiler_params=limit,
    )(place, pre, back, extras)

    said = exchange(said, ("y", "x")).reshape(YS, XS, YS, 8, tokens)
    packed = (ZS, YS, 3 * share + 32, 128)
    keep, send, small, value = pl.pallas_call(
        backward_kernel,
        out_shape=(
            VMEM(packed, f32),
            VMEM(packed, bf16),
            jax.ShapeDtypeStruct((8, tokens), f32),
            jax.ShapeDtypeStruct((8, width), f32),
        ),
        in_specs=[smem, smem, vmem, vmem] + [anywhere] * (1 + YS + XS),
        out_specs=(vmem, vmem, vmem, vmem),
        scratch_shapes=[
            VMEM((XS, group, width), bf16),
            VMEM((group, 512), bf16),
            VMEM((group, 512), bf16),
            VMEM((width, 512), f32),
            pltpu.SemaphoreType.DMA((XS, YS, 2)),
            pltpu.SemaphoreType.DMA,
        ],
        compiler_params=limit,
        cost_estimate=pl.CostEstimate(
            flops=2 * group * XS * width * 512, bytes_accessed=12 << 20, transcendentals=0
        ),
    )(place, value_bias, near(said), pre, far(embed), *landed_parts)
    terms = (keep + ahead(send, "c", 1).astype(f32)).astype(bf16)
    landed = exchange(terms.reshape(ZS * YS, *packed[2:]), ("z", "y")).reshape(packed)

    value = jnp.sum(value[:3], axis=0).reshape(ZS // XS, CS, YS, share)
    value = value.transpose(0, 2, 1, 3).reshape(width)
    totals = jnp.concatenate([value, small[:3].reshape(-1)])
    totals = sum_over(totals.reshape(-1, tokens), "c")
    totals = [totals] + [ahead(totals, "z", s) for s in range(1, ZS)]
    grad_one, grad_two, grad_value, rest = pl.pallas_call(
        finish_kernel,
        out_shape=(
            jax.ShapeDtypeStruct((share, head_cols), f32),
            jax.ShapeDtypeStruct((share, head_cols), f32),
            jax.ShapeDtypeStruct((width // tokens, tokens), f32),
            jax.ShapeDtypeStruct((2, tokens), f32),
        ),
        in_specs=[vmem] * (ZS + 1),
        out_specs=(vmem, vmem, vmem, vmem),
    )(*map(near, totals), near(landed))

    new_one = (
        (1.0 - polyak_rate) * t_one.astype(f32) + polyak_rate * q_one.astype(f32)
    ).astype(bf16)
    new_two = (
        (1.0 - polyak_rate) * t_two.astype(f32) + polyak_rate * q_two.astype(f32)
    ).astype(bf16)
    return (
        rest[1, 0],
        grad_one,
        grad_two,
        grad_value.reshape(width),
        rest[0, :1],
        new_one,
        new_two,
    )


def solution(mesh):
    fine = Mesh(mesh.devices.reshape(ZS, YS, CS, XS), ("z", "y", "c", "x"))
    in_specs = (
        P(ROWS, None, "x"),
        P(ROWS, None),
        P(ROWS, None),
        P(ROWS),
        P(ROWS, "x"),
        P(ROWS, "x"),
        P(ROWS, "x"),
        P(ROWS, "x"),
        P(ROWS, "x"),
        P("x"),
        P(),
    )
    out_specs = (P(), P(ROWS, "x"), P(ROWS, "x"), P("x"), P(), P(ROWS, "x"), P(ROWS, "x"))

    return jax.shard_map(
        on_device, mesh=fine, in_specs=in_specs, out_specs=out_specs, check_vma=False
    )
```
